128 devices in a mesh: rep: 1, r: 16 (over y, z), s: 8 (over x, core).
Axes of the slice: x: 4, y: 4, z: 4, core: 2. Of those that a mesh axis runs over, the one named last changes fastest.
Arguments:
- x: bfloat16 [128, 2048, 1152], P(('rep', 'r', 's'))
- dy: bfloat16 [128, 2048, 1152], P(('rep', 'r', 's'))
- w_gate: bfloat16 [2, 1152, 4608], P(None, 's')
- w_up: bfloat16 [2, 1152, 4608], P(None, 's')
- w_down: bfloat16 [2, 4608, 1152], P(None, 's')
Outputs:
- output 1: bfloat16 [128, 2048, 1152], P(('rep', 'r', 's'))
- output 2: bfloat16 [2, 1152, 4608], P('rep', 's')
- output 3: bfloat16 [2, 1152, 4608], P('rep', 's')
- output 4: bfloat16 [2, 4608, 1152], P('rep', 's')
All inputs are finite; a program needn't handle non-finite values.
Results may differ from the reference program's by a relative error of at most 0.018.
Values are sent between devices in bfloat16 or wider.
A program may use at most 1.5 GiB of HBM per device.

```python
import jax
import jax.numpy as jnp
from jax import lax

SEQUENCES = 128
TOKENS = 2048
D = 1152
FF = 4608
LAYERS = 2
NAMES = ("w_gate", "w_up", "w_down")
SHAPES = {"w_gate": (LAYERS, D, FF), "w_up": (LAYERS, D, FF), "w_down": (LAYERS, FF, D)}


def bump(key, n, height):
    away = (jnp.arange(n, dtype=jnp.int32) - jax.random.randint(key, (), 0, n, jnp.int32)) % n
    return jnp.where(away < n // 8, height, 1.0)


def together(key, own, strength):
    shared = jax.random.normal(key, own.shape[1:], jnp.float32)
    return (own + strength * shared) * lax.rsqrt(1 + strength * strength)


def setup_inputs(seed: int = 0, part: int = 0) -> dict:
    kx, kdy, ka, kb, kz, kf, kh, kl, *kw = jax.random.split(jax.random.key(seed), 8 + len(NAMES))
    kx, kdy, ka, kb = (jax.random.fold_in(k, part) for k in (kx, kdy, ka, kb))
    shape = (SEQUENCES, TOKENS, D)
    much_x, much_dy = jax.random.uniform(kz, (2,), jnp.float32, 0.0, 1.0)
    layers = 2.0 ** jax.random.uniform(kl, (LAYERS, 1, 1), jnp.float32, -1.0, 1.0)
    x = together(ka, jax.random.normal(kx, shape, jnp.float32), much_x) * bump(kf, D, 4.0)
    dy = together(kb, jax.random.normal(kdy, shape, jnp.float32), much_dy)
    drawn = {"x": x.astype(jnp.bfloat16), "dy": (dy * (SEQUENCES * TOKENS) ** -0.5).astype(jnp.bfloat16)}
    for key, name in zip(kw, NAMES, strict=True):
        w = jax.random.normal(key, SHAPES[name], jnp.float32) * SHAPES[name][1] ** -0.5
        drawn[name] = (w * {"w_gate": 1.0, "w_up": bump(kh, FF, 4.0), "w_down": layers}[name]).astype(jnp.bfloat16)
    return drawn


def matmul(a, w):
    return jnp.dot(a, w, preferred_element_type=jnp.float32).astype(jnp.bfloat16)


def normed(h):
    wide = h.astype(jnp.float32)
    scale = lax.rsqrt(jnp.mean(wide**2, -1, keepdims=True) + 1e-6)
    return (wide * scale).astype(jnp.bfloat16)


def layer(h, w):
    a = normed(h)
    gate = jnp.dot(a, w["w_gate"], preferred_element_type=jnp.float32)
    up = jnp.dot(a, w["w_up"], preferred_element_type=jnp.float32)
    return h + matmul((jax.nn.silu(gate) * up).astype(jnp.bfloat16), w["w_down"])


def stack(weights, h):
    return lax.scan(lambda h, w: (layer(h, w), None), h, weights)[0]


def reference(x, dy, w_gate, w_up, w_down):
    weights = dict(zip(NAMES, (w_gate, w_up, w_down), strict=True))

    def take(so_far, sequence):
        h, by_y = sequence
        _, back = jax.vjp(stack, weights, h)
        by_weights, by_h = back(by_y)
        return jax.tree.map(lambda total, term: total + term.astype(jnp.float32), so_far, by_weights), by_h

    none_yet = {name: jnp.zeros(w.shape, jnp.float32) for name, w in weights.items()}
    by_weights, by_x = lax.scan(take, none_yet, (x, dy))
    return (by_x, *(by_weights[name].astype(jnp.bfloat16) for name in NAMES))
```

```python
import functools

import jax
import jax.numpy as jnp
from jax import lax
from jax.experimental import pallas as pl
from jax.experimental.pallas import tpu as pltpu
from jax.sharding import PartitionSpec as P

RING = 4
BLOCK = 128
CHUNK = RING * BLOCK
BOTH = 2 * CHUNK
HALF = BLOCK // 2
PART = HALF // RING
VMEM_LIMIT = 66_900_000
SIDES = (1, 3)
OTHERS = (1, 2, 3)
ALL = (0, 1, 2, 3)
f32, bf16 = jnp.float32, jnp.bfloat16


def dot(a, b):
    return jnp.dot(a, b, preferred_element_type=f32)


def dot_nt(a, b):
    return lax.dot_general(a, b, (((1,), (1,)), ((), ())), preferred_element_type=f32)


def dot_tn(a, b):
    return lax.dot_general(a, b, (((0,), (0,)), ((), ())), preferred_element_type=f32)


def rows_at(start, size, unit=None):
    return pl.ds(pl.multiple_of(start, size if unit is None else unit), size)


def add_up(*terms):
    total = terms[0].astype(f32)
    for term in terms[1:]:
        total = total + term.astype(f32)
    return total.astype(bf16)


def scale_of(wide):
    return lax.rsqrt(jnp.mean(wide**2, -1, keepdims=True) + 1e-6)


def normed(h):
    wide = h.astype(f32)
    return (wide * scale_of(wide)).astype(bf16)


def on(cond):
    return pl.when(cond)


class Place:
    def __init__(self):
        r, s = lax.axis_index("r"), lax.axis_index("s")
        self.y, self.z, self.x, self.c = r // RING, lax.rem(r, RING), s // 2, lax.rem(s, 2)

    def at(self, dy=0, dz=0, dx=0, dc=0):
        y, z, x = (lax.rem(v + d, RING) for v, d in ((self.y, dy), (self.z, dz), (self.x, dx)))
        return {"r": y * RING + z, "s": x * 2 + lax.rem(self.c + dc, 2)}

    def along(self, first, step, dc=0):
        return self.at(dy=first * step, dz=(1 - first) * step, dc=dc)


def send(src, dst, send_sem, recv_sem, device):
    pltpu.make_async_remote_copy(
        src_ref=src, dst_ref=dst, send_sem=send_sem, recv_sem=recv_sem, device_id=device, device_id_type=pl.DeviceIdType.MESH
    ).start()


def drain(ref, sem):
    pltpu.make_async_copy(ref, ref, sem).wait()


def meet(devices):
    barrier = pltpu.get_barrier_semaphore()
    for device in devices:
        pl.semaphore_signal(barrier, inc=1, device_id=device, device_id_type=pl.DeviceIdType.MESH)
    pl.semaphore_wait(barrier, len(devices))


class Gather:
    def __init__(self, place, chunks, wg, wu, wd, lent, full_gu, full_d, send_sem, recv_sem):
        self.p, self.chunks = place, chunks
        self.few = chunks // 2
        self.many = chunks - self.few
        self.wg, self.wu, self.wd, self.lent, self.gu, self.d = wg, wu, wd, lent, full_gu, full_d
        self.ss, self.rs = send_sem, recv_sem
        self.rows = wg.shape[1]

    def lend(self, sem):
        for l in range(2):
            for i in range(self.few):
                send(self.wd.at[l, pl.ds((2 * i + 1) * HALF, HALF), :], self.lent.at[l, i], sem.at[0], sem.at[1], self.p.at(dc=1))
        for i in range(2):
            drain(self.lent, sem.at[i])

    def with_down(self, n, use):
        l, k = n // self.chunks, lax.rem(n, self.chunks)
        c = self.p.c
        first = c * self.few
        owned = (k >= first) & (k < first + self.many)
        start = 2 * (k - first) * HALF

        @on(owned)
        def _():
            use(self.wd.at[l, rows_at(start, HALF), :])

        @on(jnp.logical_not(owned))
        def _():
            use(self.lent.at[l, k - (1 - c) * self.many])

    def of(self, n):
        k = lax.rem(n, self.chunks)
        first = 1 - lax.rem(n, 2)
        quarter = first * self.p.y + (1 - first) * self.p.z
        return n // self.chunks, k, first, quarter

    def sems(self, step, n):
        return self.ss.at[step, lax.rem(n, 2)], self.rs.at[step, lax.rem(n, 2)]

    def own_columns(self, j, k):
        return rows_at((j * self.chunks + k) * BLOCK, BLOCK)

    def piece(self, which, n, x, quarter, part=None):
        share = 1 if part is None else 2
        offset = 0 if part is None else part
        if which == "d":
            size = PART // share
            start = x * BLOCK + self.p.c * HALF + quarter * PART + offset * size
            return self.d.at[n, rows_at(start, size), :]
        size = self.rows // share
        start = (2 * x + self.p.c) * self.rows + offset * size
        column = quarter * BLOCK + (CHUNK if which == "u" else 0)
        return self.gu.at[n, rows_at(start, size, 8), rows_at(column, BLOCK)]

    def settle(self, step, n, blocks, columns, rows):
        ss, rs = self.sems(step, n)
        for sems in (rs, ss):
            drain(self.gu.at[0, pl.ds(0, blocks * self.rows), pl.ds(0, columns * BLOCK)], sems.at[0])
            drain(self.d.at[0, pl.ds(0, rows), :], sems.at[1])

    def x1_wide(self, n):
        p = self.p
        l, k, _, _ = self.of(n)
        ss, rs = self.sems(0, n)
        for dx in SIDES:
            send(self.wg.at[l, :, self.own_columns(p.y, k)], self.piece("g", n, p.x, p.y), ss.at[0], rs.at[0], p.at(dx=dx))
            send(self.wu.at[l, :, self.own_columns(p.z, k)], self.piece("u", n, p.x, p.z), ss.at[0], rs.at[0], p.at(dx=dx))

    def x1_down(self, n):
        p = self.p
        _, _, _, q = self.of(n)
        ss, rs = self.sems(0, n)

        def use(ref):
            for dx in SIDES:
                send(ref.at[rows_at(q * PART, PART), :], self.piece("d", n, p.x, q), ss.at[1], rs.at[1], p.at(dx=dx))

        self.with_down(n, use)

    def x1(self, n):
        self.x1_wide(n)
        self.x1_down(n)

    def x2(self, n):
        p = self.p
        _, _, _, q = self.of(n)
        self.settle(0, n, 1, 4, 2 * PART)
        ss, rs = self.sems(1, n)
        for part, to in enumerate(SIDES):
            x = lax.rem(p.x + RING - to, RING)
            for which, quarter, i in (("g", p.y, 0), ("u", p.z, 0), ("d", q, 1)):
                ref = self.piece(which, n, x, quarter, part)
                send(ref, ref, ss.at[i], rs.at[i], p.at(dx=to))

    def settle_x2(self, n):
        self.settle(1, n, 1, 2, PART)

    def round(self, n, q, first, step):
        p = self.p
        return (("g", p.y, p.at(dy=step), 0), ("u", p.z, p.at(dz=step), 0), ("d", q, p.along(first, step), 1))

    def yz1(self, n):
        p = self.p
        _, _, first, q = self.of(n)
        ss, rs = self.sems(2, n)
        for step in SIDES:
            for which, quarter, to, i in self.round(n, q, first, step):
                for dx in OTHERS:
                    ref = self.piece(which, n, lax.rem(p.x + dx, RING), quarter)
                    send(ref, ref, ss.at[i], rs.at[i], to)

    def settle_yz1(self, n):
        self.settle(2, n, 3, 4, 6 * PART)

    def yz2(self, n):
        p = self.p
        _, _, first, q = self.of(n)
        ss, rs = self.sems(3, n)
        for part, step in enumerate(SIDES):
            for which, quarter, to, i in self.round(n, q, first, step):
                for dx in OTHERS:
                    ref = self.piece(which, n, lax.rem(p.x + dx, RING), lax.rem(quarter + RING - step, RING), part)
                    send(ref, ref, ss.at[i], rs.at[i], to)

    def settle_yz2(self, n):
        self.settle(3, n, 3, 2, 3 * PART)

    def device_rows(self, x, c):
        return rows_at((2 * x + c) * self.rows, self.rows, 8), rows_at((2 * x + c) * HALF, HALF)

    def own(self, n, gu, d, copy):
        l, k, _, _ = self.of(n)
        gu_rows, d_rows = self.device_rows(self.p.x, self.p.c)
        for j in ALL:
            for i, w in enumerate((self.wg, self.wu)):
                copy(w.at[l, :, self.own_columns(j, k)], gu.at[gu_rows, pl.ds(i * CHUNK + j * BLOCK, BLOCK)], 0)
        self.with_down(n, lambda ref: copy(ref, d.at[d_rows, :], 1))

    def across(self, n):
        p = self.p
        ss, rs = self.sems(4, n)
        to = p.at(dc=1)
        gu, d = self.gu.at[n], self.d.at[n]
        self.own(n, gu, d, lambda src, dst, i: send(src, dst, ss.at[i], rs.at[i], to))
        for dx in OTHERS:
            gu_rows, d_rows = self.device_rows(lax.rem(p.x + dx, RING), p.c)
            send(gu.at[gu_rows, :], gu.at[gu_rows, :], ss.at[0], rs.at[0], to)
            send(d.at[d_rows, :], d.at[d_rows, :], ss.at[1], rs.at[1], to)

    def arrived(self, n):
        self.settle(4, n, 4, 8, 4 * HALF)

    def load(self, n, slot, gu_v, d_v, sem):
        p = self.p
        gu, d = gu_v.at[slot], d_v.at[slot]
        start = lambda src, dst, i: pltpu.make_async_copy(src, dst, sem.at[slot, i]).start()
        self.own(n, gu, d, start)
        spans = [self.device_rows(p.x, 1 - p.c)]
        for dx in OTHERS:
            x = lax.rem(p.x + dx, RING)
            spans.append((rows_at(2 * x * self.rows, 2 * self.rows, 8), rows_at(x * BLOCK, BLOCK)))
        for gu_rows, d_rows in spans:
            start(self.gu.at[n, gu_rows, :], gu.at[gu_rows, :], 0)
            start(self.d.at[n, d_rows, :], d.at[d_rows, :], 1)

    def loaded(self, slot, gu_v, d_v, sem):
        drain(gu_v.at[slot], sem.at[slot, 0])
        drain(d_v.at[slot], sem.at[slot, 1])


def forward_kernel(chunks, x_ref, wg, wu, wd, full_gu, full_d, lent, kept, h_ref, a_ref, x_v, a_v, y_v, gu_v, d_v, kept_v, ss, rs, ld_sem, kept_sem, io_sem, lend_sem):
    p = Place()
    meet([p.at(dc=1)] + [p.at(**{axis: side}) for axis in ("dx", "dy", "dz") for side in SIDES])
    tokens = x_v.shape[0]
    half = tokens // 2
    tile = min(BLOCK, half)
    g = Gather(p, chunks, wg, wu, wd, lent, full_gu, full_d, ss, rs)
    x_copy = pltpu.make_async_copy(x_ref, x_v, io_sem.at[0])
    x_copy.start()
    g.x1_wide(0)
    g.lend(lend_sem)
    g.x1_down(0)
    g.x1(1)
    x_copy.wait()

    @pl.loop(0, tokens // tile)
    def _(i):
        t = rows_at(i * tile, tile)
        a_v[t, :] = normed(x_v[t, :])
        y_v[t, :] = jnp.zeros((tile, y_v.shape[1]), f32)

    g.x2(0)
    g.x2(1)
    g.settle_x2(0)
    g.yz1(0)
    g.settle_x2(1)
    g.yz1(1)
    g.x1(2)
    g.settle_yz1(0)
    g.yz2(0)
    g.x1(3)
    g.x2(2)
    g.settle_yz2(0)
    g.across(0)
    g.settle_yz1(1)
    g.yz2(1)
    g.settle_x2(2)
    g.yz1(2)
    g.x2(3)
    g.arrived(0)
    g.load(0, 0, gu_v, d_v, ld_sem)

    def part(k, i):
        slot = lax.rem(k, 2)
        t = pl.ds(i * half, half)

        @on(k > 0)
        def _():
            drain(kept_v.at[i], kept_sem.at[i])

        kept_v[i] = dot(a_v[t, :], gu_v[slot])
        pltpu.make_async_copy(kept_v.at[i], kept.at[k, t, :], kept_sem.at[i]).start()
        gate, up = kept_v[i, :, :CHUNK], kept_v[i, :, CHUNK:]
        act = (jax.nn.silu(gate) * up).astype(bf16)
        y_v[t, :] += dot(act, d_v[slot])

    @pl.loop(0, chunks)
    def _(k):
        g.settle_yz2(k + 1)
        g.across(k + 1)
        g.settle_yz1(k + 2)
        g.yz2(k + 2)
        g.settle_x2(k + 3)
        g.yz1(k + 3)
        g.x1(k + 4)
        g.loaded(lax.rem(k, 2), gu_v, d_v, ld_sem)
        part(k, 0)
        g.x2(k + 4)
        g.arrived(k + 1)

        @on(k + 1 < chunks)
        def _():
            g.load(k + 1, lax.rem(k + 1, 2), gu_v, d_v, ld_sem)

        part(k, 1)

    @pl.loop(0, tokens // tile)
    def _(i):
        t = rows_at(i * tile, tile)
        h = add_up(x_v[t, :], y_v[t, :].astype(bf16))
        x_v[t, :] = h
        a_v[t, :] = normed(h)

    h_copy = pltpu.make_async_copy(x_v, h_ref, io_sem.at[0])
    a_copy = pltpu.make_async_copy(a_v, a_ref, io_sem.at[1])
    h_copy.start()
    a_copy.start()
    g.settle_yz2(chunks + 1)
    g.settle_yz1(chunks + 2)
    g.settle_x2(chunks + 3)
    for i in range(2):
        drain(kept_v.at[i], kept_sem.at[i])
    h_copy.wait()
    a_copy.wait()


def vmem(*shape, dtype=bf16):
    return pltpu.VMEM(shape, dtype)


def dma(*shape):
    return pltpu.SemaphoreType.DMA(shape)


def call(kernel, number, ins, outs, scratch, aliases):
    any_ = pl.BlockSpec(memory_space=pl.ANY)
    return pl.pallas_call(
        kernel,
        in_specs=[any_] * len(ins),
        out_specs=[any_] * len(outs),
        out_shape=[jax.ShapeDtypeStruct(shape, dtype) for shape, dtype in outs],
        input_output_aliases=aliases,
        scratch_shapes=scratch,
        compiler_params=pltpu.CompilerParams(collective_id=number, has_side_effects=True, vmem_limit_bytes=VMEM_LIMIT),
    )(*ins)


def forward(x, wg, wu, wd, chunks):
    tokens, d = x.shape
    layers = wg.shape[0]
    n = layers * chunks
    outs = [
        ((n, d, BOTH), bf16),
        ((n, CHUNK, d), bf16),
        ((layers, chunks // 2, HALF, d), bf16),
        ((chunks, tokens, BOTH), f32),
        (x.shape, bf16),
        (x.shape, bf16),
    ]
    scratch = [vmem(tokens, d)] * 2 + [vmem(tokens, d, dtype=f32)]
    scratch += [vmem(2, d, BOTH), vmem(2, CHUNK, d), vmem(2, tokens // 2, BOTH, dtype=f32)]
    scratch += [dma(5, 2, 2)] * 2 + [dma(2, 2)] + [dma(2)] * 3
    return call(functools.partial(forward_kernel, chunks), 0, (x, wg, wu, wd), outs, scratch, {})


class Reduce:
    def __init__(self, place, chunks, own, out, bufs, sems):
        self.p, self.chunks = place, chunks
        self.own_gu, self.own_d = own
        self.out_g, self.out_u, self.out_d = out
        (self.pair_gu, self.pair_d, self.r1_gu, self.r1_d, self.s1_gu, self.s1_d, self.r2_gu, self.r2_d, self.s2_gu, self.s2_d) = bufs[:10]
        (self.f_gu, self.f_d, self.y_g, self.y_u, self.y_d, self.z_g, self.z_u, self.z_d, self.o_g, self.o_u, self.o_d) = bufs[10:]
        (self.pair_s, self.pair_r, self.s1_s, self.s1_r, self.s2_s, self.s2_r, self.y_s, self.y_r, self.z_s, self.z_r, self.o_s, self.o_r, self.l_sem, self.c_r) = sems
        self.rows = self.f_gu.shape[0]

    @staticmethod
    def scratch(rows, d, chunks):
        pair = [vmem(3, RING, rows, BOTH), vmem(3, RING, HALF, d)]
        r1, s1 = ([vmem(*lead, rows, CHUNK), vmem(*lead, HALF // 2, d)] for lead in ((2, 2), (2,)))
        r2, s2, f = ([vmem(*lead, rows, BOTH), vmem(*lead, HALF, d)] for lead in ((2, 2), (2,), ()))
        y, z, o = ([vmem(*lead, rows, BLOCK)] * 2 + [vmem(*lead, PART, d)] for lead in ((3,), (4,), ()))
        bufs = pair + r1 + s1 + r2 + s2 + f + y + z + o
        sems = [dma(3, 2)] * 2 + [dma(2), dma(2, 2)] * 2 + [dma(3)] * 7 + [dma(2 * chunks)]
        return bufs, sems

    def device_rows(self, x, c):
        return rows_at((2 * x + c) * self.rows, self.rows, 8), rows_at((2 * x + c) * HALF, HALF)

    def pair(self, q):
        p = self.p
        slot, slot3 = lax.rem(q, 2), lax.rem(q, 3)
        to = p.at(dc=1)
        for x in ALL:
            gu_rows, d_rows = self.device_rows(x, 1 - p.c)
            send(self.own_gu.at[slot, gu_rows, :], self.pair_gu.at[slot3, x], self.pair_s.at[slot3, 0], self.pair_r.at[slot3, 0], to)
            send(self.own_d.at[slot, d_rows, :], self.pair_d.at[slot3, x], self.pair_s.at[slot3, 1], self.pair_r.at[slot3, 1], to)

    def terms(self, q, x):
        slot, slot3 = lax.rem(q, 2), lax.rem(q, 3)
        gu_rows, d_rows = self.device_rows(x, self.p.c)
        return (self.own_gu[slot, gu_rows, :], self.pair_gu[slot3, x]), (self.own_d[slot, d_rows, :], self.pair_d[slot3, x])

    def x1(self, q):
        p = self.p
        slot, slot3 = lax.rem(q, 2), lax.rem(q, 3)
        for sem in (self.pair_r, self.pair_s):
            drain(self.pair_gu.at[slot3], sem.at[slot3, 0])
            drain(self.pair_d.at[slot3], sem.at[slot3, 1])
        gu, d = self.terms(q, lax.rem(p.x + 2, RING))
        for i in range(2):
            self.s1_gu[i] = add_up(*(t[:, i * CHUNK : (i + 1) * CHUNK] for t in gu))
            self.s1_d[i] = add_up(*(t[i * HALF // 2 : (i + 1) * HALF // 2] for t in d))
        for i, dx in enumerate(SIDES):
            send(self.s1_gu.at[i], self.r1_gu.at[slot, i], self.s1_s.at[0], self.s1_r.at[slot, 0], p.at(dx=dx))
            send(self.s1_d.at[i], self.r1_d.at[slot, i], self.s1_s.at[1], self.s1_r.at[slot, 1], p.at(dx=dx))

    def x2(self, q):
        p = self.p
        slot = lax.rem(q, 2)
        drain(self.r1_gu.at[slot], self.s1_r.at[slot, 0])
        drain(self.r1_d.at[slot], self.s1_r.at[slot, 1])
        drain(self.s1_gu, self.s1_s.at[0])
        drain(self.s1_d, self.s1_s.at[1])
        for i, dx in enumerate(SIDES):
            gu, d = self.terms(q, lax.rem(p.x + dx, RING))
            for j in range(2):
                columns, rows = slice(j * CHUNK, (j + 1) * CHUNK), slice(j * HALF // 2, (j + 1) * HALF // 2)
                self.s2_gu[i, :, columns] = add_up(*(t[:, columns] for t in gu), *((self.r1_gu[slot, i],) if i == j else ()))
                self.s2_d[i, rows, :] = add_up(*(t[rows] for t in d), *((self.r1_d[slot, i],) if i == j else ()))
        for i, dx in enumerate(SIDES):
            send(self.s2_gu.at[i], self.r2_gu.at[slot, i], self.s2_s.at[0], self.s2_r.at[slot, 0], p.at(dx=dx))
            send(self.s2_d.at[i], self.r2_d.at[slot, i], self.s2_s.at[1], self.s2_r.at[slot, 1], p.at(dx=dx))

    def of(self, q):
        p = self.p
        first = 1 - lax.rem(q, 2)
        return first, first * p.y + (1 - first) * p.z, first * p.z + (1 - first) * p.y

    def mine(self, quarter):
        return rows_at(quarter * BLOCK, BLOCK)

    def yz1(self, q):
        p = self.p
        slot = lax.rem(q, 2)
        drain(self.r2_gu.at[slot], self.s2_r.at[slot, 0])
        drain(self.r2_d.at[slot], self.s2_r.at[slot, 1])
        drain(self.s2_gu, self.s2_s.at[0])
        drain(self.s2_d, self.s2_s.at[1])
        gu, d = self.terms(q, p.x)
        self.f_gu[...] = add_up(*gu, self.r2_gu[slot, 0], self.r2_gu[slot, 1])
        self.f_d[...] = add_up(*d, self.r2_d[slot, 0], self.r2_d[slot, 1])
        first, along, _ = self.of(q)
        for i, step in enumerate(OTHERS):
            y, z, a = (lax.rem(v + step, RING) for v in (p.y, p.z, along))
            send(self.f_gu.at[:, self.mine(y)], self.y_g.at[i], self.y_s.at[0], self.y_r.at[0], p.at(dy=step))
            send(self.f_gu.at[:, self.mine(RING + z)], self.y_u.at[i], self.y_s.at[1], self.y_r.at[1], p.at(dz=step))
            send(self.f_d.at[rows_at(a * PART, PART), :], self.y_d.at[i], self.y_s.at[2], self.y_r.at[2], p.along(first, step))

    def yz2(self, q):
        p = self.p
        came = (self.y_g, self.y_u, self.y_d)
        for i, ref in enumerate(came):
            drain(ref, self.y_r.at[i])
            drain(ref, self.y_s.at[i])
        first, along, over = self.of(q)
        own = (self.f_gu[:, self.mine(p.y)], self.f_gu[:, self.mine(RING + p.z)], self.f_d[rows_at(along * PART, PART), :])
        sums = ((self.z_g, p.z), (self.z_u, p.y), (self.z_d, over))
        for (ref, place), term, more in zip(sums, own, came):
            ref[place] = add_up(term, *(more[i] for i in range(3)))
        for step in OTHERS:
            for i, ((ref, place), to) in enumerate(zip(sums, (p.at(dz=step), p.at(dy=step), p.along(1 - first, step)))):
                send(ref.at[place], ref.at[place], self.z_s.at[i], self.z_r.at[i], to)

    def out(self, q):
        p = self.p
        l, k = 1 - q // self.chunks, lax.rem(q, self.chunks)
        _, along, _ = self.of(q)
        column = lambda j: rows_at((j * self.chunks + k) * BLOCK, BLOCK)
        rows = self.chunks * HALF
        row = k * BLOCK + p.c * HALF + along * PART
        g, u = self.out_g.at[l, :, column(p.y)], self.out_u.at[l, :, column(p.z)]
        return (g, u, self.out_d.at[l, rows_at(lax.rem(row, rows), PART), :]), row // rows == p.c

    def lends(self, q):
        row = lax.rem(q, self.chunks) * BLOCK + (1 - self.p.c) * HALF
        return row // (self.chunks * HALF) == self.p.c

    def yz3(self, q):
        p = self.p
        sums = (self.z_g, self.z_u, self.z_d)
        done = (self.o_g, self.o_u, self.o_d)
        for i, ref in enumerate(sums):
            drain(ref.at[pl.ds(0, 3)], self.z_r.at[i])
            drain(ref.at[pl.ds(0, 3)], self.z_s.at[i])
        for ref, total in zip(sums, done):
            total[...] = add_up(*(ref[i] for i in ALL))
        first, _, _ = self.of(q)
        out, owned = self.out(q)

        def spread(i, to):
            pltpu.make_async_copy(done[i], out[i], self.l_sem.at[i]).start()
            for step in OTHERS:
                send(done[i], out[i], self.o_s.at[i], self.o_r.at[i], to(step))

        spread(0, lambda step: p.at(dy=step))
        spread(1, lambda step: p.at(dz=step))

        @on(owned)
        def _():
            spread(2, lambda step: p.along(first, step))

        @on(jnp.logical_not(owned))
        def _():
            for step in ALL:
                send(done[2], out[2], self.o_s.at[2], self.c_r.at[q], p.along(first, step, dc=1))

    def finish(self, q):
        _, owned = self.out(q)

        def settle(i, ref, total):
            drain(ref, self.o_r.at[i])
            drain(ref, self.o_s.at[i])
            drain(total, self.l_sem.at[i])

        settle(0, self.y_g, self.o_g)
        settle(1, self.y_u, self.o_u)

        @on(owned)
        def _():
            settle(2, self.y_d, self.o_d)

        @on(jnp.logical_not(owned))
        def _():
            drain(self.z_d, self.o_s.at[2])

        @on(self.lends(q))
        def _():
            drain(self.z_d, self.c_r.at[q])


def backward_kernel(chunks, a_ref, dy_ref, h_ref, x_ref, kept, wg, wu, wd, lent, full_gu_in, full_d_in, full_gu, full_d, dx_ref, out_g, out_u, out_d, *scratch):
    a_v, dy_v, da_v, gu_v, d_v, dgu_v, act_v, kept_v, *own = scratch[:10]
    (ss, rs, ld_sem, kept_sem, io_sem), bufs, sems = scratch[10:15], scratch[15:36], scratch[36:]
    p = Place()
    meet([p.at(dc=1)] + [p.at(dx=side) for side in SIDES] + [p.at(**{axis: step}, dc=dc) for axis in ("dy", "dz") for step in OTHERS for dc in range(2)])
    tokens, d = a_v.shape
    half, tile = tokens // 2, tokens // 4
    small = min(BLOCK, tile)
    g = Gather(p, chunks, wg, wu, wd, lent, full_gu, full_d, ss, rs)
    r = Reduce(p, chunks, own, (out_g, out_u, out_d), bufs, sems)
    total = 2 * chunks

    def fetch(ref, i):
        return pltpu.make_async_copy(ref, (a_v, dy_v)[i], io_sem.at[i])

    def number(q):
        return (1 - q // chunks) * chunks + lax.rem(q, chunks)

    def keep(t):
        b = lax.rem(t, 2)
        return pltpu.make_async_copy(kept.at[t // 4, rows_at(lax.rem(t, 4) * tile, tile), :], kept_v.at[b], kept_sem.at[b])

    def through_norm(then):
        @pl.loop(0, tokens // small)
        def _(i):
            t = rows_at(i * small, small)
            wide = a_v[t, :].astype(f32)
            scale = scale_of(wide)
            hat = wide * scale
            da = da_v[t, :].astype(bf16).astype(f32)
            back = scale * (da - hat * jnp.mean(da * hat, -1, keepdims=True))
            dy_v[t, :] = add_up(dy_v[t, :], back.astype(bf16))
            da_v[t, :] = jnp.zeros((small, d), f32)
            then(t)

    def through_gate(t, gate, up, slot):
        dact = dot_nt(dy_v[t, :], d_v[slot]).astype(bf16).astype(f32)
        sig = jax.nn.sigmoid(gate)
        silu = gate * sig
        act_v[t, :] = (silu * up).astype(bf16)
        dgu_v[t, :CHUNK] = (dact * up * (sig * (1 + gate * (1 - sig)))).astype(bf16)
        dgu_v[t, CHUNK:] = (dact * silu).astype(bf16)

    def gate_part(q, slot, i):
        @on(q < chunks)
        def _():
            t = pl.ds(i * half, half)
            gu = dot(a_v[t, :], gu_v[slot])
            through_gate(t, gu[:, :CHUNK], gu[:, CHUNK:], slot)

        @on((q >= chunks) & (q < total))
        def _():
            @pl.loop(0, 2)
            def _(j):
                n = (q - chunks) * 4 + 2 * i + j

                @on(n + 1 < 4 * chunks)
                def _():
                    keep(n + 1).start()

                keep(n).wait()
                t = rows_at((2 * i + j) * tile, tile)
                b = lax.rem(n, 2)
                through_gate(t, kept_v[b, :, :CHUNK], kept_v[b, :, CHUNK:], slot)

    fetch(a_ref, 0).start()
    fetch(dy_ref, 1).start()
    g.load(chunks, 0, gu_v, d_v, ld_sem)

    @pl.loop(0, tokens // small)
    def _(i):
        da_v[rows_at(i * small, small), :] = jnp.zeros((small, d), f32)

    fetch(a_ref, 0).wait()
    fetch(dy_ref, 1).wait()

    @pl.loop(0, total + 3)
    def _(q):
        slot = lax.rem(q, 2)
        busy = q < total
        ahead = chunks + q + 2
        gathers = q + 2 < chunks
        one = (q >= 1) & (q <= total)
        two = (q >= 2) & (q <= total + 1)
        three = q >= 3

        @on(one)
        def _():
            r.x1(q - 1)

        @on(gathers & (q >= 2))
        def _():
            g.x1(ahead)

        @on(q == chunks)
        def _():
            fetch(h_ref, 0).wait()

            def then(t):
                pltpu.make_async_copy(x_ref.at[t, :], a_v.at[t, :], io_sem.at[0]).start()

            through_norm(then)
            fetch(x_ref, 0).wait()

            @pl.loop(0, tokens // small)
            def _(i):
                t = rows_at(i * small, small)
                a_v[t, :] = normed(a_v[t, :])

        @on(q == total)
        def _():
            fetch(x_ref, 0).wait()
            through_norm(lambda t: None)
            pltpu.make_async_copy(dy_v, dx_ref, io_sem.at[0]).start()

        @on(busy)
        def _():
            g.loaded(slot, gu_v, d_v, ld_sem)

        gate_part(q, slot, 0)

        @on(three)
        def _():
            r.yz3(q - 3)

        @on(gathers & (q >= 2))
        def _():
            g.x2(ahead)

        @on((q + 1 < chunks) & (q >= 1))
        def _():
            g.settle_yz2(ahead - 1)

        @on(q + 1 < chunks)
        def _():
            g.across(ahead - 1)

        gate_part(q, slot, 1)

        @on(gathers & (q >= 2))
        def _():
            g.settle_x2(ahead)

        @on(gathers & (q >= 1))
        def _():
            g.yz1(ahead)

        @on(two)
        def _():
            r.yz1(q - 2)

        @on(busy)
        def _():
            own[0][slot] = dot_tn(a_v[...], dgu_v[...]).astype(bf16)

        @on(q == chunks - 1)
        def _():
            fetch(h_ref, 0).start()
            keep(0).start()

        @on(q == total - 1)
        def _():
            fetch(x_ref, 0).start()

        @on(one)
        def _():
            r.x2(q - 1)

        @on(q + 1 < chunks)
        def _():
            g.arrived(ahead - 1)

        @on(q + 1 < total)
        def _():
            g.load(number(q + 1), 1 - slot, gu_v, d_v, ld_sem)

        @on(busy)
        def _():
            own[1][slot] = dot_tn(act_v[...], dy_v[...]).astype(bf16)

        @on(three)
        def _():
            r.finish(q - 3)

        @on(busy)
        def _():
            r.pair(q)

        @on(two)
        def _():
            r.yz2(q - 2)

        @on(gathers & (q >= 1))
        def _():
            g.settle_yz1(ahead)

        @on(gathers)
        def _():
            g.yz2(ahead)

        @on(busy)
        def _():
            @pl.loop(0, 2)
            def _(i):
                t = rows_at(i * half, half)
                da_v[t, :] += dot_nt(dgu_v[t, :], gu_v[slot])

    pltpu.make_async_copy(dy_v, dx_ref, io_sem.at[0]).wait()


def backward(a, dy, h, x, kept, wg, wu, wd, lent, full_gu, full_d, chunks):
    tokens, d = x.shape
    ins = (a, dy, h, x, kept, wg, wu, wd, lent, full_gu, full_d)
    outs = [(v.shape, bf16) for v in (full_gu, full_d, x, wg, wu, wd)]
    weights = [vmem(2, d, BOTH), vmem(2, CHUNK, d)]
    scratch = [vmem(tokens, d)] * 2 + [vmem(tokens, d, dtype=f32)] + weights
    scratch += [vmem(tokens, BOTH), vmem(tokens, CHUNK), vmem(2, tokens // 4, BOTH, dtype=f32)] + weights
    scratch += [dma(5, 2, 2)] * 2 + [dma(2, 2)] + [dma(2)] * 2
    bufs, sems = Reduce.scratch(wg.shape[1], d, chunks)
    aliases = {len(ins) - 2: 0, len(ins) - 1: 1}
    return call(functools.partial(backward_kernel, chunks), 1, ins, outs, scratch + bufs + sems, aliases)


def solution(mesh):
    def step(x, dy, wg, wu, wd):
        chunks = wg.shape[2] // CHUNK
        full_gu, full_d, lent, kept, h, a = forward(x[0], wg, wu, wd, chunks)
        _, _, dx, *out = backward(a, dy[0], h, x[0], kept, wg, wu, wd, lent, full_gu, full_d, chunks)
        return dx[None], *out

    states, cut = P(("rep", "r", "s"), None, None), P(None, "s", None)
    return jax.shard_map(
        step,
        mesh=mesh,
        in_specs=(states, states) + (cut,) * 3,
        out_specs=(states,) + (P("rep", "s", None),) * 3,
        check_vma=False,
    )
```

```python
import functools

import jax
import jax.numpy as jnp
from jax import lax
from jax.experimental import pallas as pl
from jax.experimental.pallas import tpu as pltpu
from jax.sharding import PartitionSpec as P

RING = 4
BLOCK = 128
CHUNK = RING * BLOCK
BOTH = 2 * CHUNK
HALF = BLOCK // 2
PART = HALF // RING
VMEM_LIMIT = 66_900_000
SIDES = (1, 3)
OTHERS = (1, 2, 3)
ALL = (0, 1, 2, 3)
f32, bf16 = jnp.float32, jnp.bfloat16


def dot(a, b):
    return jnp.dot(a, b, preferred_element_type=f32)


def dot_nt(a, b):
    return lax.dot_general(a, b, (((1,), (1,)), ((), ())), preferred_element_type=f32)


def dot_tn(a, b):
    return lax.dot_general(a, b, (((0,), (0,)), ((), ())), preferred_element_type=f32)


def rows_at(start, size, unit=None):
    return pl.ds(pl.multiple_of(start, size if unit is None else unit), size)


def add_up(*terms):
    total = terms[0].astype(f32)
    for term in terms[1:]:
        total = total + term.astype(f32)
    return total.astype(bf16)


def scale_of(wide):
    return lax.rsqrt(jnp.mean(wide**2, -1, keepdims=True) + 1e-6)


def normed(h):
    wide = h.astype(f32)
    return (wide * scale_of(wide)).astype(bf16)


def on(cond):
    return pl.when(cond)


class Place:
    def __init__(self):
        r, s = lax.axis_index("r"), lax.axis_index("s")
        self.y, self.z, self.x, self.c = r // RING, lax.rem(r, RING), s // 2, lax.rem(s, 2)

    def at(self, dy=0, dz=0, dx=0, dc=0):
        y, z, x = (lax.rem(v + d, RING) for v, d in ((self.y, dy), (self.z, dz), (self.x, dx)))
        return {"r": y * RING + z, "s": x * 2 + lax.rem(self.c + dc, 2)}

    def along(self, first, step, dc=0):
        return self.at(dy=first * step, dz=(1 - first) * step, dc=dc)


def send(src, dst, send_sem, recv_sem, device):
    pltpu.make_async_remote_copy(
        src_ref=src, dst_ref=dst, send_sem=send_sem, recv_sem=recv_sem, device_id=device, device_id_type=pl.DeviceIdType.MESH
    ).start()


def drain(ref, sem):
    pltpu.make_async_copy(ref, ref, sem).wait()


def meet(devices):
    barrier = pltpu.get_barrier_semaphore()
    for device in devices:
        pl.semaphore_signal(barrier, inc=1, device_id=device, device_id_type=pl.DeviceIdType.MESH)
    pl.semaphore_wait(barrier, len(devices))


class Gather:
    def __init__(self, place, chunks, wg, wu, wd, lent, full_gu, full_d, send_sem, recv_sem):
        self.p, self.chunks = place, chunks
        self.few = chunks // 2
        self.many = chunks - self.few
        self.wg, self.wu, self.wd, self.lent, self.gu, self.d = wg, wu, wd, lent, full_gu, full_d
        self.ss, self.rs = send_sem, recv_sem
        self.rows = wg.shape[1]

    def lend(self, sem):
        for l in range(2):
            for i in range(self.few):
                send(self.wd.at[l, pl.ds((2 * i + 1) * HALF, HALF), :], self.lent.at[l, i], sem.at[0], sem.at[1], self.p.at(dc=1))

    def settle_lend(self, sem):
        for i in range(2):
            drain(self.lent, sem.at[i])

    def with_down(self, n, use):
        l, k = n // self.chunks, lax.rem(n, self.chunks)
        c = self.p.c
        first = c * self.few
        owned = (k >= first) & (k < first + self.many)
        start = 2 * (k - first) * HALF

        @on(owned)
        def _():
            use(self.wd.at[l, rows_at(start, HALF), :])

        @on(jnp.logical_not(owned))
        def _():
            use(self.lent.at[l, k - (1 - c) * self.many])

    def of(self, n):
        k = lax.rem(n, self.chunks)
        first = self.p.c
        quarter = first * self.p.y + (1 - first) * self.p.z
        return n // self.chunks, k, first, quarter

    def sems(self, step, n):
        return self.ss.at[step, lax.rem(n, 2)], self.rs.at[step, lax.rem(n, 2)]

    def own_columns(self, j, k):
        return rows_at((j * self.chunks + k) * BLOCK, BLOCK)

    def piece(self, which, n, x, quarter, part=None):
        share = 1 if part is None else 2
        offset = 0 if part is None else part
        if which == "d":
            size = PART // share
            start = x * BLOCK + self.p.c * HALF + quarter * PART + offset * size
            return self.d.at[n, rows_at(start, size), :]
        size = self.rows // share
        start = (2 * x + self.p.c) * self.rows + offset * size
        column = quarter * BLOCK + (CHUNK if which == "u" else 0)
        return self.gu.at[n, rows_at(start, size, 8), rows_at(column, BLOCK)]

    def settle(self, step, n, blocks, columns, rows):
        ss, rs = self.sems(step, n)
        for sems in (rs, ss):
            drain(self.gu.at[0, pl.ds(0, blocks * self.rows), pl.ds(0, columns * BLOCK)], sems.at[0])
            drain(self.d.at[0, pl.ds(0, rows), :], sems.at[1])

    def x1_wide(self, n):
        p = self.p
        l, k, _, _ = self.of(n)
        ss, rs = self.sems(0, n)
        for dx in SIDES:
            send(self.wg.at[l, :, self.own_columns(p.y, k)], self.piece("g", n, p.x, p.y), ss.at[0], rs.at[0], p.at(dx=dx))
            send(self.wu.at[l, :, self.own_columns(p.z, k)], self.piece("u", n, p.x, p.z), ss.at[0], rs.at[0], p.at(dx=dx))

    def x1_down(self, n):
        p = self.p
        _, _, _, q = self.of(n)
        ss, rs = self.sems(0, n)

        def use(ref):
            for dx in SIDES:
                send(ref.at[rows_at(q * PART, PART), :], self.piece("d", n, p.x, q), ss.at[1], rs.at[1], p.at(dx=dx))

        self.with_down(n, use)

    def x1(self, n):
        self.x1_wide(n)
        self.x1_down(n)

    def x2(self, n):
        p = self.p
        _, _, _, q = self.of(n)
        self.settle(0, n, 1, 4, 2 * PART)
        ss, rs = self.sems(1, n)
        for part, to in enumerate(SIDES):
            x = lax.rem(p.x + RING - to, RING)
            for which, quarter, i in (("g", p.y, 0), ("u", p.z, 0), ("d", q, 1)):
                ref = self.piece(which, n, x, quarter, part)
                send(ref, ref, ss.at[i], rs.at[i], p.at(dx=to))

    def settle_x2(self, n):
        self.settle(1, n, 1, 2, PART)

    def round(self, n, q, first, step):
        p = self.p
        return (("g", p.y, p.at(dy=step), 0), ("u", p.z, p.at(dz=step), 0), ("d", q, p.along(first, step), 1))

    def yz1(self, n):
        p = self.p
        _, _, first, q = self.of(n)
        ss, rs = self.sems(2, n)
        for step in SIDES:
            for which, quarter, to, i in self.round(n, q, first, step):
                for dx in OTHERS:
                    ref = self.piece(which, n, lax.rem(p.x + dx, RING), quarter)
                    send(ref, ref, ss.at[i], rs.at[i], to)

    def settle_yz1(self, n):
        self.settle(2, n, 3, 4, 6 * PART)

    def yz2(self, n):
        p = self.p
        _, _, first, q = self.of(n)
        ss, rs = self.sems(3, n)
        for part, step in enumerate(SIDES):
            for which, quarter, to, i in self.round(n, q, first, step):
                for dx in OTHERS:
                    ref = self.piece(which, n, lax.rem(p.x + dx, RING), lax.rem(quarter + RING - step, RING), part)
                    send(ref, ref, ss.at[i], rs.at[i], to)

    def settle_yz2(self, n):
        self.settle(3, n, 3, 2, 3 * PART)

    def device_rows(self, x, c):
        return rows_at((2 * x + c) * self.rows, self.rows, 8), rows_at((2 * x + c) * HALF, HALF)

    def own(self, n, gu, d, copy):
        l, k, _, _ = self.of(n)
        gu_rows, d_rows = self.device_rows(self.p.x, self.p.c)
        for j in ALL:
            for i, w in enumerate((self.wg, self.wu)):
                copy(w.at[l, :, self.own_columns(j, k)], gu.at[gu_rows, pl.ds(i * CHUNK + j * BLOCK, BLOCK)], 0)
        self.with_down(n, lambda ref: copy(ref, d.at[d_rows, :], 1))

    def across(self, n):
        p = self.p
        ss, rs = self.sems(4, n)
        to = p.at(dc=1)
        gu, d = self.gu.at[n], self.d.at[n]
        self.own(n, gu, d, lambda src, dst, i: send(src, dst, ss.at[i], rs.at[i], to))
        for dx in OTHERS:
            gu_rows, d_rows = self.device_rows(lax.rem(p.x + dx, RING), p.c)
            send(gu.at[gu_rows, :], gu.at[gu_rows, :], ss.at[0], rs.at[0], to)
            send(d.at[d_rows, :], d.at[d_rows, :], ss.at[1], rs.at[1], to)

    def arrived(self, n):
        self.settle(4, n, 4, 8, 4 * HALF)

    def load(self, n, slot, gu_v, d_v, sem):
        p = self.p
        gu, d = gu_v.at[slot], d_v.at[slot]
        start = lambda src, dst, i: pltpu.make_async_copy(src, dst, sem.at[slot, i]).start()
        self.own(n, gu, d, start)
        spans = [self.device_rows(p.x, 1 - p.c)]
        for dx in OTHERS:
            x = lax.rem(p.x + dx, RING)
            spans.append((rows_at(2 * x * self.rows, 2 * self.rows, 8), rows_at(x * BLOCK, BLOCK)))
        for gu_rows, d_rows in spans:
            start(self.gu.at[n, gu_rows, :], gu.at[gu_rows, :], 0)
            start(self.d.at[n, d_rows, :], d.at[d_rows, :], 1)

    def loaded(self, slot, gu_v, d_v, sem):
        drain(gu_v.at[slot], sem.at[slot, 0])
        drain(d_v.at[slot], sem.at[slot, 1])


def vmem(*shape, dtype=bf16):
    return pltpu.VMEM(shape, dtype)


def dma(*shape):
    return pltpu.SemaphoreType.DMA(shape)


class Reduce:
    def __init__(self, place, chunks, kind, own, out, bufs, sems):
        self.p, self.chunks, self.kind, self.own, self.out = place, chunks, kind, own, out
        self.pair_v, self.r1, self.s1, self.r2, self.s2, self.f, self.y, self.z, self.o = bufs
        self.pair_s, self.pair_r, self.s1_s, self.s1_r, self.s2_s, self.s2_r, self.y_s, self.y_r, self.z_s, self.z_r, self.o_s, self.o_r, self.l_sem, self.c_r = sems
        self.rows = self.f.shape[1]

    @staticmethod
    def scratch(kind, rows, d, chunks):
        block, axis = ([rows, CHUNK], 1) if kind < 2 else ([HALF, d], 0)

        def buf(lead, parts):
            shape = list(block)
            shape[axis] //= parts
            return vmem(*lead, *shape)

        r1, s1, r2, s2 = (buf(lead, parts) for parts in (2, 1) for lead in ((2, 2), (2,)))
        bufs = [buf((3, RING), 1), r1, s1, r2, s2, buf((2,), 1), buf((2, 3), RING), buf((2, RING), RING), buf((2,), RING)]
        sems = [dma(3)] * 2 + [dma(1), dma(2)] * 2 + [dma(2)] * 7 + [dma(2 * chunks)]
        return bufs, sems

    def part(self, i, parts):
        if self.kind < 2:
            return slice(None), rows_at(i * (CHUNK // parts), CHUNK // parts)
        return rows_at(i * (HALF // parts), HALF // parts), slice(None)

    def device_rows(self, x, c):
        return rows_at((2 * x + c) * self.rows, self.rows, PART)

    def pair(self, q):
        p = self.p
        slot, slot3 = lax.rem(q, 2), lax.rem(q, 3)
        for x in ALL:
            send(self.own.at[slot, self.device_rows(x, 1 - p.c), :], self.pair_v.at[slot3, x], self.pair_s.at[slot3], self.pair_r.at[slot3], p.at(dc=1))

    def terms(self, q, x, i, parts):
        rows, columns = self.part(i, parts)
        own = self.own.at[lax.rem(q, 2), self.device_rows(x, self.p.c), :]
        return own[rows, columns], self.pair_v.at[lax.rem(q, 3), x][rows, columns]

    def x1(self, q):
        p = self.p
        slot, slot3 = lax.rem(q, 2), lax.rem(q, 3)
        for sem in (self.pair_r, self.pair_s):
            drain(self.pair_v.at[slot3], sem.at[slot3])
        for i in range(2):
            self.s1[i] = add_up(*self.terms(q, lax.rem(p.x + 2, RING), i, 2))
        for i, dx in enumerate(SIDES):
            send(self.s1.at[i], self.r1.at[slot, i], self.s1_s.at[0], self.s1_r.at[slot], p.at(dx=dx))

    def x2(self, q):
        p = self.p
        slot = lax.rem(q, 2)
        drain(self.r1.at[slot], self.s1_r.at[slot])
        drain(self.s1, self.s1_s.at[0])
        for i, dx in enumerate(SIDES):
            for j in range(2):
                more = (self.r1[slot, i],) if i == j else ()
                self.s2.at[i][self.part(j, 2)] = add_up(*self.terms(q, lax.rem(p.x + dx, RING), j, 2), *more)
            send(self.s2.at[i], self.r2.at[slot, i], self.s2_s.at[0], self.s2_r.at[slot], p.at(dx=dx))

    def of(self, q):
        p = self.p
        first = (1, 0, p.c)[self.kind]
        return first, first * p.y + (1 - first) * p.z, first * p.z + (1 - first) * p.y

    def yz1(self, q):
        p = self.p
        slot = lax.rem(q, 2)
        drain(self.r2.at[slot], self.s2_r.at[slot])
        drain(self.s2, self.s2_s.at[0])
        self.f[slot] = add_up(*self.terms(q, p.x, 0, 1), *(self.r2[slot, i] for i in range(2)))
        first, along, _ = self.of(q)
        for i, step in enumerate(OTHERS):
            src = self.f.at[(slot, *self.part(lax.rem(along + step, RING), RING))]
            send(src, self.y.at[slot, i], self.y_s.at[slot], self.y_r.at[slot], p.along(first, step))

    def yz2(self, q):
        p = self.p
        slot = lax.rem(q, 2)
        for sem in (self.y_r, self.y_s):
            drain(self.y.at[slot], sem.at[slot])
        first, along, over = self.of(q)
        self.z[slot, over] = add_up(self.f.at[slot][self.part(along, RING)], *(self.y[slot, i] for i in range(3)))
        for step in OTHERS:
            send(self.z.at[slot, over], self.z.at[slot, over], self.z_s.at[slot], self.z_r.at[slot], p.along(1 - first, step))

    def place_of(self, q):
        p = self.p
        l, k = 1 - q // self.chunks, lax.rem(q, self.chunks)
        _, along, _ = self.of(q)
        if self.kind < 2:
            return self.out.at[l, :, rows_at((along * self.chunks + k) * BLOCK, BLOCK)], None
        rows = self.chunks * HALF
        row = k * BLOCK + p.c * HALF + along * PART
        return self.out.at[l, rows_at(lax.rem(row, rows), PART), :], row // rows == p.c

    def lends(self, q):
        row = lax.rem(q, self.chunks) * BLOCK + (1 - self.p.c) * HALF
        return row // (self.chunks * HALF) == self.p.c

    def yz3(self, q):
        p = self.p
        slot = lax.rem(q, 2)
        for sem in (self.z_r, self.z_s):
            drain(self.z.at[slot, pl.ds(0, 3)], sem.at[slot])
        self.o[slot] = add_up(*(self.z[slot, i] for i in ALL))
        first, _, _ = self.of(q)
        out, owned = self.place_of(q)

        def spread():
            pltpu.make_async_copy(self.o.at[slot], out, self.l_sem.at[slot]).start()
            for step in OTHERS:
                send(self.o.at[slot], out, self.o_s.at[slot], self.o_r.at[slot], p.along(first, step))

        if owned is None:
            spread()
            return
        on(owned)(spread)

        @on(jnp.logical_not(owned))
        def _():
            for step in ALL:
                send(self.o.at[slot], out, self.o_s.at[slot], self.c_r.at[q], p.along(first, step, dc=1))

    def finish(self, q):
        slot = lax.rem(q, 2)
        _, owned = self.place_of(q)

        def settle():
            for sem in (self.o_r, self.o_s):
                drain(self.y.at[slot], sem.at[slot])
            drain(self.o.at[slot], self.l_sem.at[slot])

        if owned is None:
            settle()
            return
        on(owned)(settle)

        @on(jnp.logical_not(owned))
        def _():
            drain(self.z.at[slot], self.o_s.at[slot])

        @on(self.lends(q))
        def _():
            drain(self.z.at[slot], self.c_r.at[q])


def kernel(chunks, x_ref, dy_ref, wg, wu, wd, full_gu, full_d, lent, kept, h_ref, dx_ref, out_g, out_u, out_d, *scratch):
    a_v, dy_v, da_v, gu_v, d_v, dgu_v, act_v, kept_v, own, (ss, rs, ld_sem, kept_sem, io_sem, lend_sem), reduces = scratch
    p = Place()
    meet([p.at(dc=1)] + [p.at(dx=side) for side in SIDES] + [p.at(**{axis: step}, dc=dc) for axis in ("dy", "dz") for step in OTHERS for dc in range(2)])
    tokens, d = a_v.shape
    half = tokens // 2
    small = min(BLOCK, half)
    g = Gather(p, chunks, wg, wu, wd, lent, full_gu, full_d, ss, rs)
    parts = [Reduce(p, chunks, kind, own[kind], (out_g, out_u, out_d)[kind], *reduces[kind]) for kind in (2, 0, 1)]
    total = 2 * chunks

    def tiles(start, stop, count, use):
        steps = tokens // small

        @pl.loop(start * steps // count, stop * steps // count)
        def _(i):
            use(rows_at(i * small, small))

    x_copy = pltpu.make_async_copy(x_ref, dy_v, io_sem.at[0])
    x_copy.start()
    g.lend(lend_sem)
    g.x1_wide(0)
    x_copy.wait()

    def first_norm(t):
        a_v[t, :] = normed(dy_v[t, :])
        da_v[t, :] = jnp.zeros((small, d), f32)

    tiles(0, 1, 4, first_norm)
    g.settle_lend(lend_sem)
    g.x1_down(0)
    g.x1(1)
    tiles(1, 3, 4, first_norm)
    g.x2(0)
    tiles(3, 4, 4, first_norm)
    g.x2(1)
    g.settle_x2(0)
    g.yz1(0)
    g.settle_x2(1)
    g.yz1(1)
    g.x1(2)
    g.settle_yz1(0)
    g.yz2(0)
    g.x1(3)
    g.x2(2)
    g.settle_yz2(0)
    g.across(0)
    g.settle_yz1(1)
    g.yz2(1)
    g.settle_x2(2)
    g.yz1(2)
    g.x2(3)
    g.arrived(0)
    g.load(0, 0, gu_v, d_v, ld_sem)

    def gather_on(n):
        @on(n + 1 < total)
        def _():
            g.settle_yz2(n + 1)
            g.across(n + 1)

        @on(n + 2 < total)
        def _():
            g.settle_yz1(n + 2)
            g.yz2(n + 2)

        @on(n + 3 < total)
        def _():
            g.settle_x2(n + 3)
            g.yz1(n + 3)

        @on(n + 4 < total)
        def _():
            g.x1(n + 4)

    def gather_more(n):
        @on(n + 4 < total)
        def _():
            g.x2(n + 4)

        @on(n + 1 < total)
        def _():
            g.arrived(n + 1)

    def forward_part(k, i):
        slot = lax.rem(k, 2)
        t = rows_at(i * half, half)

        @on(k > 0)
        def _():
            drain(kept_v.at[i], kept_sem.at[i])

        kept_v[i] = dot(a_v[t, :], gu_v[slot])
        pltpu.make_async_copy(kept_v.at[i], kept.at[k, t, :], kept_sem.at[i]).start()
        gate, up = kept_v[i, :, :CHUNK], kept_v[i, :, CHUNK:]
        act = (jax.nn.silu(gate) * up).astype(bf16)
        da_v[t, :] += dot(act, d_v[slot])

    @pl.loop(0, chunks)
    def _(k):
        gather_on(k)
        g.loaded(lax.rem(k, 2), gu_v, d_v, ld_sem)
        forward_part(k, 0)
        gather_more(k)
        g.load(k + 1, lax.rem(k + 1, 2), gu_v, d_v, ld_sem)
        forward_part(k, 1)

    def between(t):
        h = add_up(dy_v[t, :], da_v[t, :].astype(bf16))
        a_v[t, :] = normed(h)
        da_v[t, :] = jnp.zeros((small, d), f32)
        dgu_v[t, :] = h[:, :BOTH]
        act_v[t, : d - BOTH] = h[:, BOTH:]
        pltpu.make_async_copy(dy_ref.at[t, :], dy_v.at[t, :], io_sem.at[0]).start()
        pltpu.make_async_copy(dgu_v.at[t, :], h_ref.at[t, :BOTH], io_sem.at[1]).start()
        pltpu.make_async_copy(act_v.at[t, : d - BOTH], h_ref.at[t, BOTH:], io_sem.at[1]).start()

    tiles(0, 1, 1, between)
    drain(dy_v, io_sem.at[0])
    drain(a_v, io_sem.at[1])
    for i in range(2):
        drain(kept_v.at[i], kept_sem.at[i])

    def each(step, q):
        for part in parts:
            getattr(part, step)(q)

    def fetch(ref):
        return pltpu.make_async_copy(ref, a_v, io_sem.at[0])

    def number(q):
        return (1 - q // chunks) * chunks + lax.rem(q, chunks)

    def keep(t):
        b = lax.rem(t, 2)
        return pltpu.make_async_copy(kept.at[t // 2, rows_at(b * half, half), :], kept_v.at[b], kept_sem.at[b])

    def through_norm(start, stop, then):
        def use(t):
            wide = a_v[t, :].astype(f32)
            scale = scale_of(wide)
            hat = wide * scale
            da = da_v[t, :].astype(bf16).astype(f32)
            back = scale * (da - hat * jnp.mean(da * hat, -1, keepdims=True))
            dy_v[t, :] = add_up(dy_v[t, :], back.astype(bf16))
            da_v[t, :] = jnp.zeros((small, d), f32)
            then(t)

        tiles(start, stop, 2, use)

    def through_gate(t, gate, up, slot):
        dact = dot_nt(dy_v[t, :], d_v[slot]).astype(bf16).astype(f32)
        sig = jax.nn.sigmoid(gate)
        silu = gate * sig
        act_v[t, :] = (silu * up).astype(bf16)
        dgu_v[t, :CHUNK] = (dact * up * (sig * (1 + gate * (1 - sig)))).astype(bf16)
        dgu_v[t, CHUNK:] = (dact * silu).astype(bf16)

    def da_tile(t, slot):
        da_v[t, :] += dot_nt(dgu_v[t, :], gu_v[slot])

    def gate_part(q, slot, i):
        k = lax.rem(q, chunks)

        def layer1(joined):
            t = rows_at(i * half, half)
            if joined:
                da_tile(t, 1 - slot)
            gu = dot(a_v[t, :], gu_v[slot])
            through_gate(t, gu[:, :CHUNK], gu[:, CHUNK:], slot)

        def layer0(joined):
            n = (q - chunks) * 2 + i
            keep(n).wait()
            t = rows_at(i * half, half)
            if joined:
                da_tile(t, 1 - slot)
            through_gate(t, kept_v[i, :, :CHUNK], kept_v[i, :, CHUNK:], slot)

            @on(n + 2 < 2 * chunks)
            def _():
                keep(n + 2).start()

        for joined in (False, True):
            on((q < chunks) & ((k > 0) == joined))(functools.partial(layer1, joined))
            on((q >= chunks) & (q < total) & ((k > 0) == joined))(functools.partial(layer0, joined))

    @pl.loop(0, total + 4)
    def _(q):
        slot, side = lax.rem(q, 2), lax.rem(q + chunks, 2)
        busy = q < total
        ahead = chunks + q
        one = (q >= 1) & (q <= total)
        two = (q >= 2) & (q <= total + 1)
        three = (q >= 3) & (q <= total + 2)

        @on(q >= 4)
        def _():
            each("finish", q - 4)

        @on(three)
        def _():
            each("yz2", q - 3)

        @on((q == chunks) | (q == total))
        def _():
            @pl.loop(0, 2)
            def _(i):
                da_tile(rows_at(i * half, half), 1 - side)

        @on(q == chunks)
        def _():
            fetch(h_ref).wait()

            def then(t):
                pltpu.make_async_copy(x_ref.at[t, :], a_v.at[t, :], io_sem.at[0]).start()

            through_norm(0, 2, then)
            fetch(x_ref).wait()

            def again(t):
                a_v[t, :] = normed(a_v[t, :])

            tiles(0, 1, 1, again)

        gather_on(ahead)

        @on(busy)
        def _():
            g.loaded(side, gu_v, d_v, ld_sem)

        @pl.loop(0, 2)
        def _(i):
            @on(one & (i == 1))
            def _():
                each("x1", q - 1)

            gate_part(q, side, i)

        @on(three)
        def _():
            each("yz3", q - 3)

        @on(two)
        def _():
            each("yz1", q - 2)

        gather_more(ahead)

        @on(q + 1 < total)
        def _():
            g.load(number(q + 1), 1 - side, gu_v, d_v, ld_sem)

        @on(busy)
        def _():
            own[2][slot] = dot_tn(act_v[...], dy_v[...]).astype(bf16)
            parts[0].pair(q)

        @on(q == total)
        def _():
            fetch(x_ref).wait()
            through_norm(0, 1, lambda t: None)

        @on(one)
        def _():
            each("x2", q - 1)

        @on(busy)
        def _():
            both = dot_tn(a_v[...], dgu_v[...]).astype(bf16)
            own[0][slot] = both[:, :CHUNK]
            own[1][slot] = both[:, CHUNK:]
            for part in parts[1:]:
                part.pair(q)

        @on(q == total)
        def _():
            through_norm(1, 2, lambda t: None)
            pltpu.make_async_copy(dy_v, dx_ref, io_sem.at[0]).start()

        @on(q == chunks - 1)
        def _():
            fetch(h_ref).start()
            keep(0).start()
            keep(1).start()

        @on(q == total - 1)
        def _():
            fetch(x_ref).start()

    pltpu.make_async_copy(dy_v, dx_ref, io_sem.at[0]).wait()


def call(x, dy, wg, wu, wd, chunks):
    tokens, d = x.shape
    layers, rows, _ = wg.shape
    n = layers * chunks
    shapes = [(n, d, BOTH), (n, CHUNK, d), (layers, chunks // 2, HALF, d), (chunks, tokens, BOTH), x.shape, x.shape, wg.shape, wu.shape, wd.shape]
    outs = [jax.ShapeDtypeStruct(shape, f32 if shape == (chunks, tokens, BOTH) else bf16) for shape in shapes]
    scratch = [vmem(tokens, d)] * 2 + [vmem(tokens, d, dtype=f32), vmem(2, d, BOTH), vmem(2, CHUNK, d)]
    scratch += [vmem(tokens, BOTH), vmem(tokens, CHUNK), vmem(2, tokens // 2, BOTH, dtype=f32)]
    scratch += [[vmem(2, d, CHUNK)] * 2 + [vmem(2, CHUNK, d)]]
    scratch += [[dma(5, 2, 2)] * 2 + [dma(2, 2)] + [dma(2)] * 3]
    scratch += [[Reduce.scratch(kind, rows, d, chunks) for kind in range(3)]]
    any_ = pl.BlockSpec(memory_space=pl.ANY)
    ins = (x, dy, wg, wu, wd)
    return pl.pallas_call(
        functools.partial(kernel, chunks),
        in_specs=[any_] * len(ins),
        out_specs=[any_] * len(outs),
        out_shape=outs,
        scratch_shapes=scratch,
        compiler_params=pltpu.CompilerParams(collective_id=0, has_side_effects=True, vmem_limit_bytes=VMEM_LIMIT),
        name="stack",
    )(*ins)


def solution(mesh):
    def step(x, dy, wg, wu, wd):
        dx, *out = call(x[0], dy[0], wg, wu, wd, wg.shape[2] // CHUNK)[5:]
        return dx[None], *out

    states, cut = P(("rep", "r", "s"), None, None), P(None, "s", None)
    return jax.shard_map(
        step,
        mesh=mesh,
        in_specs=(states, states) + (cut,) * 3,
        out_specs=(states,) + (P("rep", "s", None),) * 3,
        check_vma=False,
    )
```

```python
import functools

import jax
import jax.numpy as jnp
from jax import lax
from jax.experimental import pallas as pl
from jax.experimental.pallas import tpu as pltpu
from jax.sharding import PartitionSpec as P

RING = 4
BLOCK = 128
CHUNK = RING * BLOCK
BOTH = 2 * CHUNK
HALF = BLOCK // 2
PART = HALF // RING
VMEM_LIMIT = 66_900_000
SIDES = (1, 3)
OTHERS = (1, 2, 3)
ALL = (0, 1, 2, 3)
KINDS = (0, 1)
WIDE, DOWN = (0,), (1,)
f32, bf16 = jnp.float32, jnp.bfloat16


def dot(a, b):
    return jnp.dot(a, b, preferred_element_type=f32)


def dot_nt(a, b):
    return lax.dot_general(a, b, (((1,), (1,)), ((), ())), preferred_element_type=f32)


def dot_tn(a, b):
    return lax.dot_general(a, b, (((0,), (0,)), ((), ())), preferred_element_type=f32)


def rows_at(start, size, unit=None):
    return pl.ds(pl.multiple_of(start, size if unit is None else unit), size)


def add_up(*terms):
    total = terms[0].astype(f32)
    for term in terms[1:]:
        total = total + term.astype(f32)
    return total.astype(bf16)


def scale_of(wide):
    return lax.rsqrt(jnp.mean(wide**2, -1, keepdims=True) + 1e-6)


def normed(h):
    wide = h.astype(f32)
    return (wide * scale_of(wide)).astype(bf16)


def on(cond):
    return pl.when(cond)


class Place:
    def __init__(self):
        r, s = lax.axis_index("r"), lax.axis_index("s")
        self.y, self.z, self.x, self.c = r // RING, lax.rem(r, RING), s // 2, lax.rem(s, 2)

    def at(self, dy=0, dz=0, dx=0, dc=0):
        y, z, x = (lax.rem(v + d, RING) for v, d in ((self.y, dy), (self.z, dz), (self.x, dx)))
        return {"r": y * RING + z, "s": x * 2 + lax.rem(self.c + dc, 2)}

    def along(self, first, step, dc=0):
        return self.at(dy=first * step, dz=(1 - first) * step, dc=dc)


def send(src, dst, send_sem, recv_sem, device):
    pltpu.make_async_remote_copy(
        src_ref=src, dst_ref=dst, send_sem=send_sem, recv_sem=recv_sem, device_id=device, device_id_type=pl.DeviceIdType.MESH
    ).start()


def drain(ref, sem):
    pltpu.make_async_copy(ref, ref, sem).wait()


def meet(devices):
    barrier = pltpu.get_barrier_semaphore()
    for device in devices:
        pl.semaphore_signal(barrier, inc=1, device_id=device, device_id_type=pl.DeviceIdType.MESH)
    pl.semaphore_wait(barrier, len(devices))


class Gather:
    def __init__(self, place, chunks, wg, wu, wd, lent, full_gu, full_d, send_sem, recv_sem):
        self.p, self.chunks = place, chunks
        self.few = chunks // 2
        self.many = chunks - self.few
        self.wg, self.wu, self.wd, self.lent, self.gu, self.d = wg, wu, wd, lent, full_gu, full_d
        self.ss, self.rs = send_sem, recv_sem
        self.rows = wg.shape[1]
        self.total = wg.shape[0] * chunks

    def lend(self, sem):
        for l in range(2):
            for i in range(self.few):
                send(self.wd.at[l, pl.ds((2 * i + 1) * HALF, HALF), :], self.lent.at[l, i], sem.at[0], sem.at[1], self.p.at(dc=1))

    def settle_lend(self, sem):
        for i in range(2):
            drain(self.lent, sem.at[i])

    def with_down(self, n, use):
        l, k = n // self.chunks, lax.rem(n, self.chunks)
        c = self.p.c
        first = c * self.few
        owned = (k >= first) & (k < first + self.many)
        start = 2 * (k - first) * HALF

        @on(owned)
        def _():
            use(self.wd.at[l, rows_at(start, HALF), :])

        @on(jnp.logical_not(owned))
        def _():
            use(self.lent.at[l, k - (1 - c) * self.many])

    def of(self, n):
        k = lax.rem(n, self.chunks)
        first = self.p.c
        quarter = first * self.p.y + (1 - first) * self.p.z
        return n // self.chunks, k, first, quarter

    def sems(self, step, n):
        return self.ss.at[step, lax.rem(n, 2)], self.rs.at[step, lax.rem(n, 2)]

    def own_columns(self, j, k):
        return rows_at((j * self.chunks + k) * BLOCK, BLOCK)

    def piece(self, which, n, slots, quarter, part=None):
        share = 1 if part is None else 2
        offset = 0 if part is None else part
        if which == "d":
            size = PART // share
            return self.d.at[n, slots, self.p.c, rows_at(quarter * PART + offset * size, size), :]
        size = self.rows // share
        column = quarter * BLOCK + (CHUNK if which == "u" else 0)
        return self.gu.at[n, slots, self.p.c, pl.ds(offset * size, size), rows_at(column, BLOCK)]

    def settle(self, step, n, kinds, blocks, columns, rows):
        ss, rs = self.sems(step, n)
        refs = self.gu.at[0, pl.ds(0, blocks), 0, :, pl.ds(0, columns * BLOCK)], self.d.at[0, pl.ds(0, blocks), 0, pl.ds(0, rows), :]
        for i in kinds:
            for sems in (rs, ss):
                drain(refs[i], sems.at[i])

    def x1_wide(self, n):
        p = self.p
        l, k, _, _ = self.of(n)
        ss, rs = self.sems(0, n)
        for dx in SIDES:
            slot = RING - dx
            send(self.wg.at[l, :, self.own_columns(p.y, k)], self.piece("g", n, slot, p.y), ss.at[0], rs.at[0], p.at(dx=dx))
            send(self.wu.at[l, :, self.own_columns(p.z, k)], self.piece("u", n, slot, p.z), ss.at[0], rs.at[0], p.at(dx=dx))

    def x1_down(self, n):
        p = self.p
        _, _, _, q = self.of(n)
        ss, rs = self.sems(0, n)

        def use(ref):
            for dx in SIDES:
                send(ref.at[rows_at(q * PART, PART), :], self.piece("d", n, RING - dx, q), ss.at[1], rs.at[1], p.at(dx=dx))

        self.with_down(n, use)

    def x1(self, n):
        self.x1_wide(n)
        self.x1_down(n)

    def x2(self, n, kinds=KINDS):
        p = self.p
        _, _, _, q = self.of(n)
        self.settle(0, n, kinds, 1, 4, 2 * PART)
        ss, rs = self.sems(1, n)
        for part, to in enumerate(SIDES):
            for which, quarter, i in (("g", p.y, 0), ("u", p.z, 0), ("d", q, 1)):
                if i in kinds:
                    src, dst = (self.piece(which, n, slot, quarter, part) for slot in (RING - to, 2))
                    send(src, dst, ss.at[i], rs.at[i], p.at(dx=to))

    def round(self, n, kinds, step):
        p = self.p
        _, _, first, q = self.of(n)
        pieces = (("g", p.y, p.at(dy=step), 0), ("u", p.z, p.at(dz=step), 0), ("d", q, p.along(first, step), 1))
        return [piece for piece in pieces if piece[-1] in kinds]

    def yz1(self, n, kinds=KINDS):
        p = self.p
        self.settle(1, n, kinds, 1, 2, PART)
        ss, rs = self.sems(2, n)
        for step in SIDES:
            for which, quarter, to, i in self.round(n, kinds, step):
                ref = self.piece(which, n, pl.ds(1, 3), quarter)
                send(ref, ref, ss.at[i], rs.at[i], to)

    def yz2(self, n, kinds=KINDS):
        p = self.p
        self.settle(2, n, kinds, 3, 4, 2 * PART)
        ss, rs = self.sems(3, n)
        for part, step in enumerate(SIDES):
            for which, quarter, to, i in self.round(n, kinds, step):
                ref = self.piece(which, n, pl.ds(1, 3), lax.rem(quarter + RING - step, RING), part)
                send(ref, ref, ss.at[i], rs.at[i], to)

    def own(self, n, kinds, places, copy):
        l, k, _, _ = self.of(n)
        if 0 in kinds:
            for j in ALL:
                for i, w in enumerate((self.wg, self.wu)):
                    copy(w.at[l, :, self.own_columns(j, k)], places[0].at[:, pl.ds(i * CHUNK + j * BLOCK, BLOCK)], 0)
        if 1 in kinds:
            self.with_down(n, lambda ref: copy(ref, places[1], 1))

    def across(self, n, kinds=KINDS):
        c = self.p.c
        self.settle(3, n, kinds, 3, 2, PART)
        ss, rs = self.sems(4, n)
        to = self.p.at(dc=1)
        full = self.gu.at[n], self.d.at[n]
        self.own(n, kinds, [ref.at[0, c] for ref in full], lambda src, dst, i: send(src, dst, ss.at[i], rs.at[i], to))
        for i in kinds:
            ref = full[i].at[pl.ds(1, 3), c]
            send(ref, ref, ss.at[i], rs.at[i], to)

    def load(self, n, slot, into, sem, kinds=KINDS):
        p = self.p
        on(n < self.total)(lambda: self.settle(4, n, kinds, 4, 8, HALF))
        n = lax.rem(n, self.total)
        full = self.gu.at[n], self.d.at[n]
        sizes = self.rows, HALF
        place = lambda i, x, c: into[i].at[slot, rows_at((2 * x + c) * sizes[i], sizes[i], PART), :]
        start = lambda src, dst, i: pltpu.make_async_copy(src, dst, sem.at[slot, i]).start()
        self.own(n, kinds, [place(i, p.x, p.c) for i in KINDS], start)
        for i in kinds:
            start(full[i].at[0, 1 - p.c], place(i, p.x, 1 - p.c), i)
            for dx in OTHERS:
                for c in range(2):
                    start(full[i].at[dx, c], place(i, lax.rem(p.x + dx, RING), c), i)


def vmem(*shape, dtype=bf16):
    return pltpu.VMEM(shape, dtype)


def dma(*shape):
    return pltpu.SemaphoreType.DMA(shape)


class Reduce:
    def __init__(self, place, chunks, kind, own, out, bufs, sems):
        self.p, self.chunks, self.kind, self.own, self.out = place, chunks, kind, own, out
        self.pair_v, self.r1, self.s1, self.r2, self.s2, self.f, self.y, self.z, self.o = bufs
        self.pair_s, self.pair_r, self.s1_s, self.s1_r, self.s2_s, self.s2_r, self.y_s, self.y_r, self.z_s, self.z_r, self.o_s, self.o_r, self.l_sem, self.c_r = sems
        self.rows = self.f.shape[1]

    @staticmethod
    def scratch(kind, rows, d, chunks):
        block, axis = ([rows, CHUNK], 1) if kind < 2 else ([HALF, d], 0)

        def buf(lead, parts):
            shape = list(block)
            shape[axis] //= parts
            return vmem(*lead, *shape)

        r1, s1, r2, s2 = (buf(lead, parts) for parts in (2, 1) for lead in ((2, 2), (2,)))
        bufs = [buf((3, RING), 1), r1, s1, r2, s2, buf((2,), 1), buf((2, 3), RING), buf((2, RING), RING), buf((2,), RING)]
        sems = [dma(3)] * 2 + [dma(1), dma(2)] * 2 + [dma(2)] * 7 + [dma(2 * chunks)]
        return bufs, sems

    def part(self, i, parts):
        if self.kind < 2:
            return slice(None), rows_at(i * (CHUNK // parts), CHUNK // parts)
        return rows_at(i * (HALF // parts), HALF // parts), slice(None)

    def device_rows(self, x, c):
        return rows_at((2 * x + c) * self.rows, self.rows, PART)

    def pair(self, q):
        p = self.p
        slot, slot3 = lax.rem(q, 2), lax.rem(q, 3)
        for x in ALL:
            send(self.own.at[slot, self.device_rows(x, 1 - p.c), :], self.pair_v.at[slot3, x], self.pair_s.at[slot3], self.pair_r.at[slot3], p.at(dc=1))

    def terms(self, q, x, i, parts):
        rows, columns = self.part(i, parts)
        own = self.own.at[lax.rem(q, 2), self.device_rows(x, self.p.c), :]
        return own[rows, columns], self.pair_v.at[lax.rem(q, 3), x][rows, columns]

    def x1(self, q):
        p = self.p
        slot, slot3 = lax.rem(q, 2), lax.rem(q, 3)
        for sem in (self.pair_r, self.pair_s):
            drain(self.pair_v.at[slot3], sem.at[slot3])
        for i in range(2):
            self.s1[i] = add_up(*self.terms(q, lax.rem(p.x + 2, RING), i, 2))
        for i, dx in enumerate(SIDES):
            send(self.s1.at[i], self.r1.at[slot, i], self.s1_s.at[0], self.s1_r.at[slot], p.at(dx=dx))

    def x2(self, q):
        p = self.p
        slot = lax.rem(q, 2)
        drain(self.r1.at[slot], self.s1_r.at[slot])
        drain(self.s1, self.s1_s.at[0])
        for i, dx in enumerate(SIDES):
            for j in range(2):
                more = (self.r1[slot, i],) if i == j else ()
                self.s2.at[i][self.part(j, 2)] = add_up(*self.terms(q, lax.rem(p.x + dx, RING), j, 2), *more)
            send(self.s2.at[i], self.r2.at[slot, i], self.s2_s.at[0], self.s2_r.at[slot], p.at(dx=dx))

    def of(self, q):
        p = self.p
        first = (1, 0, p.c)[self.kind]
        return first, first * p.y + (1 - first) * p.z, first * p.z + (1 - first) * p.y

    def yz1(self, q):
        p = self.p
        slot = lax.rem(q, 2)
        drain(self.r2.at[slot], self.s2_r.at[slot])
        drain(self.s2, self.s2_s.at[0])
        self.f[slot] = add_up(*self.terms(q, p.x, 0, 1), *(self.r2[slot, i] for i in range(2)))
        first, along, _ = self.of(q)
        for i, step in enumerate(OTHERS):
            src = self.f.at[(slot, *self.part(lax.rem(along + step, RING), RING))]
            send(src, self.y.at[slot, i], self.y_s.at[slot], self.y_r.at[slot], p.along(first, step))

    def yz2(self, q):
        p = self.p
        slot = lax.rem(q, 2)
        for sem in (self.y_r, self.y_s):
            drain(self.y.at[slot], sem.at[slot])
        first, along, over = self.of(q)
        self.z[slot, over] = add_up(self.f.at[slot][self.part(along, RING)], *(self.y[slot, i] for i in range(3)))
        for step in OTHERS:
            send(self.z.at[slot, over], self.z.at[slot, over], self.z_s.at[slot], self.z_r.at[slot], p.along(1 - first, step))

    def place_of(self, q):
        p = self.p
        l, k = 1 - q // self.chunks, lax.rem(q, self.chunks)
        _, along, _ = self.of(q)
        if self.kind < 2:
            return self.out.at[l, :, rows_at((along * self.chunks + k) * BLOCK, BLOCK)], None
        rows = self.chunks * HALF
        row = k * BLOCK + p.c * HALF + along * PART
        return self.out.at[l, rows_at(lax.rem(row, rows), PART), :], row // rows == p.c

    def lends(self, q):
        row = lax.rem(q, self.chunks) * BLOCK + (1 - self.p.c) * HALF
        return row // (self.chunks * HALF) == self.p.c

    def yz3(self, q):
        p = self.p
        slot = lax.rem(q, 2)
        for sem in (self.z_r, self.z_s):
            drain(self.z.at[slot, pl.ds(0, 3)], sem.at[slot])
        self.o[slot] = add_up(*(self.z[slot, i] for i in ALL))
        first, _, _ = self.of(q)
        out, owned = self.place_of(q)

        def spread():
            pltpu.make_async_copy(self.o.at[slot], out, self.l_sem.at[slot]).start()
            for step in OTHERS:
                send(self.o.at[slot], out, self.o_s.at[slot], self.o_r.at[slot], p.along(first, step))

        if owned is None:
            spread()
            return
        on(owned)(spread)

        @on(jnp.logical_not(owned))
        def _():
            for step in ALL:
                send(self.o.at[slot], out, self.o_s.at[slot], self.c_r.at[q], p.along(first, step, dc=1))

    def finish(self, q):
        slot = lax.rem(q, 2)
        _, owned = self.place_of(q)

        def settle():
            for sem in (self.o_r, self.o_s):
                drain(self.y.at[slot], sem.at[slot])
            drain(self.o.at[slot], self.l_sem.at[slot])

        if owned is None:
            settle()
            return
        on(owned)(settle)

        @on(jnp.logical_not(owned))
        def _():
            drain(self.z.at[slot], self.o_s.at[slot])

        @on(self.lends(q))
        def _():
            drain(self.z.at[slot], self.c_r.at[q])


def kernel(chunks, x_ref, dy_ref, wg, wu, wd, full_gu, full_d, lent, kept, h_ref, spill, dx_ref, out_g, out_u, out_d, *scratch):
    a_v, dy_v, da_v, gu_v, d_v, dgu_v, act_v, kept_v, own, (ss, rs, ld_sem, kept_sem, io_sem, lend_sem), reduces = scratch
    p = Place()
    meet([p.at(dc=1)] + [p.at(dx=side) for side in SIDES] + [p.at(**{axis: step}, dc=dc) for axis in ("dy", "dz") for step in OTHERS for dc in range(2)])
    tokens, d = a_v.shape
    half = tokens // 2
    small = min(BLOCK, half)
    g = Gather(p, chunks, wg, wu, wd, lent, full_gu, full_d, ss, rs)
    parts = [Reduce(p, chunks, kind, own[kind], (out_g, out_u, out_d)[kind], *reduces[kind]) for kind in (2, 0, 1)]
    total = 2 * chunks

    def tiles(start, stop, count, use):
        steps = tokens // small

        @pl.loop(start * steps // count, stop * steps // count)
        def _(i):
            use(rows_at(i * small, small))

    x_copy = pltpu.make_async_copy(x_ref, dy_v, io_sem.at[0])
    x_copy.start()
    g.lend(lend_sem)
    g.x1_wide(0)
    x_copy.wait()

    def first_norm(t):
        a_v[t, :] = normed(dy_v[t, :])
        da_v[t, :] = jnp.zeros((small, d), f32)

    into = (gu_v, d_v)
    tiles(0, 1, 4, first_norm)
    g.settle_lend(lend_sem)
    g.x1_down(0)
    tiles(1, 3, 4, first_norm)
    g.x2(0, WIDE)
    g.x2(0, DOWN)
    g.x1(1)
    tiles(3, 4, 4, first_norm)
    g.yz1(0, WIDE)
    g.yz1(0, DOWN)
    g.x2(1)
    g.x1(2)
    g.yz2(0, WIDE)
    g.yz2(0, DOWN)
    g.yz1(1)
    g.x2(2)
    g.x1(3)
    g.across(0, WIDE)
    g.across(0, DOWN)
    g.yz1(2)
    g.load(0, 0, into, ld_sem, WIDE)
    g.load(0, 0, into, ld_sem, DOWN)
    g.yz2(1)
    g.x2(3)
    g.x1(4)

    def loaded(n, i):
        drain(into[i].at[lax.rem(n, 2)], ld_sem.at[lax.rem(n, 2), i])

    def gather_on(n):
        for i, step in enumerate((g.across, g.yz2, g.yz1, g.x2, g.x1)):
            on(n + i + 1 < total)(functools.partial(step, n + i + 1))

    def forward_part(k, i):
        slot = lax.rem(k, 2)
        t = rows_at(i * half, half)

        @on(k > 0)
        def _():
            drain(kept_v.at[i], kept_sem.at[i])

        kept_v[i] = dot(a_v[t, :], gu_v[slot])
        pltpu.make_async_copy(kept_v.at[i], kept.at[k, t, :], kept_sem.at[i]).start()
        gate, up = kept_v[i, :, :CHUNK], kept_v[i, :, CHUNK:]
        act = (jax.nn.silu(gate) * up).astype(bf16)
        on(i == 0)(lambda: loaded(k, 1))
        da_v[t, :] += dot(act, d_v[slot])

    @pl.loop(0, chunks)
    def _(k):
        on(k > 0)(lambda: gather_on(k))
        loaded(k, 0)

        @pl.loop(0, 2)
        def _(i):
            @on(i == 1)
            def _():
                on(k == 0)(lambda: gather_on(k))
                on(k > 0)(lambda: g.load(k + 1, lax.rem(k + 1, 2), into, ld_sem))

            forward_part(k, i)

        on(k == 0)(lambda: g.load(k + 1, lax.rem(k + 1, 2), into, ld_sem))

    def between(t):
        h = add_up(dy_v[t, :], da_v[t, :].astype(bf16))
        dy_v[t, :] = h
        a_v[t, :] = normed(h)
        da_v[t, :] = jnp.zeros((small, d), f32)
        pltpu.make_async_copy(dy_v.at[t, :], h_ref.at[t, :], io_sem.at[1]).start()

    tiles(0, 1, 1, between)
    drain(dy_v, io_sem.at[1])
    dy_copy = pltpu.make_async_copy(dy_ref, dy_v, io_sem.at[0])
    dy_copy.start()
    for i in range(2):
        drain(kept_v.at[i], kept_sem.at[i])

    def each(step, q):
        for part in parts:
            getattr(part, step)(q)

    def fetch(ref):
        return pltpu.make_async_copy(ref, a_v, io_sem.at[0])

    def keep(t):
        b = lax.rem(t, 2)
        return pltpu.make_async_copy(kept.at[t // 2, rows_at(b * half, half), :], kept_v.at[b], kept_sem.at[b])

    def through_norm(start, stop, then):
        def use(t):
            wide = a_v[t, :].astype(f32)
            scale = scale_of(wide)
            hat = wide * scale
            da = da_v[t, :].astype(bf16).astype(f32)
            back = scale * (da - hat * jnp.mean(da * hat, -1, keepdims=True))
            dy_v[t, :] = add_up(dy_v[t, :], back.astype(bf16))
            da_v[t, :] = jnp.zeros((small, d), f32)
            then(t)

        tiles(start, stop, 2, use)

    def through_gate(t, gate, up, slot):
        dact = dot_nt(dy_v[t, :], d_v[slot]).astype(bf16).astype(f32)
        sig = jax.nn.sigmoid(gate)
        silu = gate * sig
        act_v[t, :] = (silu * up).astype(bf16)
        dgu_v[t, :CHUNK] = (dact * up * (sig * (1 + gate * (1 - sig)))).astype(bf16)
        dgu_v[t, CHUNK:] = (dact * silu).astype(bf16)

    def da_tile(t, slot):
        da_v[t, :] += dot_nt(dgu_v[t, :], gu_v[slot])

    def gate_part(q, slot, i):
        k = lax.rem(q, chunks)

        def layer1(joined):
            t = rows_at(i * half, half)
            if joined:
                da_tile(t, 1 - slot)
            gu = dot(a_v[t, :], gu_v[slot])
            if not joined:
                on(i == 0)(dy_copy.wait)
            through_gate(t, gu[:, :CHUNK], gu[:, CHUNK:], slot)

        def layer0(joined):
            n = (q - chunks) * 2 + i
            keep(n).wait()
            t = rows_at(i * half, half)
            if joined:
                da_tile(t, 1 - slot)
            through_gate(t, kept_v[i, :, :CHUNK], kept_v[i, :, CHUNK:], slot)

            @on(n + 2 < 2 * chunks)
            def _():
                keep(n + 2).start()

        joins = (k > 0) & (q != total - 1)
        for joined in (False, True):
            on((q < chunks) & (joins == joined))(functools.partial(layer1, joined))
            on((q >= chunks) & (q < total) & (joins == joined))(functools.partial(layer0, joined))

    away_copy = pltpu.make_async_copy(dgu_v, spill, io_sem.at[1])

    def back_copy(i):
        t = rows_at(i * half, half)
        return pltpu.make_async_copy(spill.at[t, :], dgu_v.at[t, :], kept_sem.at[i])

    @pl.loop(0, total + 4)
    def _(q):
        slot, side = lax.rem(q, 2), lax.rem(q + chunks, 2)
        busy = q < total
        ahead = chunks + q
        one = (q >= 1) & (q <= total)
        two = (q >= 2) & (q <= total + 1)
        three = (q >= 3) & (q <= total + 2)

        @on(q >= 4)
        def _():
            each("finish", q - 4)

        @on(three)
        def _():
            each("yz2", q - 3)

        @pl.loop(0, jnp.where(q == total, 4, jnp.where(q == chunks, 2, 0)))
        def _(i):
            j = lax.rem(i, 2)
            on((q == total) & (i == 1))(lambda: each("x1", q - 1))

            @on(i == 3)
            def _():
                each("yz3", q - 3)
                each("yz1", q - 2)
                each("x2", q - 1)

            on(i >= 2)(back_copy(j).wait)
            da_tile(rows_at(j * half, half), jnp.where(i < 2, 1 - side, side))
            on((q == total) & (i < 2))(back_copy(j).start)

        on(q == total - 1)(away_copy.wait)

        @on(q == chunks)
        def _():
            fetch(h_ref).wait()

            def then(t):
                pltpu.make_async_copy(x_ref.at[t, :], a_v.at[t, :], io_sem.at[0]).start()

            through_norm(0, 2, then)
            fetch(x_ref).wait()

            def again(t):
                a_v[t, :] = normed(a_v[t, :])

            tiles(0, 1, 1, again)

        gather_on(ahead)

        @on(busy)
        def _():
            loaded(ahead, 0)
            loaded(ahead, 1)

        @pl.loop(0, 2)
        def _(i):
            @on((q >= 1) & (q < total) & (i == 1))
            def _():
                each("x1", q - 1)

            gate_part(q, side, i)

        on(q == total - 2)(away_copy.start)

        @on(three & (q != total))
        def _():
            each("yz3", q - 3)

        @on(two & (q != total))
        def _():
            each("yz1", q - 2)

        @on(q + 1 < total)
        def _():
            g.load(ahead + 1, 1 - side, into, ld_sem)

        @on(busy)
        def _():
            own[2][slot] = dot_tn(act_v[...], dy_v[...]).astype(bf16)
            parts[0].pair(q)

        @on(q == total)
        def _():
            fetch(x_ref).wait()
            through_norm(0, 1, lambda t: None)

        @on(one & (q != total))
        def _():
            each("x2", q - 1)

        @on(busy)
        def _():
            both = dot_tn(a_v[...], dgu_v[...]).astype(bf16)
            own[0][slot] = both[:, :CHUNK]
            own[1][slot] = both[:, CHUNK:]
            for part in parts[1:]:
                part.pair(q)

        @on(q == total)
        def _():
            through_norm(1, 2, lambda t: None)
            pltpu.make_async_copy(dy_v, dx_ref, io_sem.at[0]).start()

        @on(q == chunks - 1)
        def _():
            fetch(h_ref).start()
            keep(0).start()
            keep(1).start()

        @on(q == total - 1)
        def _():
            fetch(x_ref).start()

    pltpu.make_async_copy(dy_v, dx_ref, io_sem.at[0]).wait()


def call(x, dy, wg, wu, wd, chunks):
    tokens, d = x.shape
    layers, rows, _ = wg.shape
    n = layers * chunks
    shapes = [(n, RING, 2, rows, BOTH), (n, RING, 2, HALF, d), (layers, chunks // 2, HALF, d), (chunks, tokens, BOTH), x.shape, (tokens, BOTH), x.shape, wg.shape, wu.shape, wd.shape]
    outs = [jax.ShapeDtypeStruct(shape, f32 if shape == (chunks, tokens, BOTH) else bf16) for shape in shapes]
    scratch = [vmem(tokens, d)] * 2 + [vmem(tokens, d, dtype=f32), vmem(2, d, BOTH), vmem(2, CHUNK, d)]
    scratch += [vmem(tokens, BOTH), vmem(tokens, CHUNK), vmem(2, tokens // 2, BOTH, dtype=f32)]
    scratch += [[vmem(2, d, CHUNK)] * 2 + [vmem(2, CHUNK, d)]]
    scratch += [[dma(5, 2, 2)] * 2 + [dma(2, 2)] + [dma(2)] * 3]
    scratch += [[Reduce.scratch(kind, rows, d, chunks) for kind in range(3)]]
    any_ = pl.BlockSpec(memory_space=pl.ANY)
    ins = (x, dy, wg, wu, wd)
    return pl.pallas_call(
        functools.partial(kernel, chunks),
        in_specs=[any_] * len(ins),
        out_specs=[any_] * len(outs),
        out_shape=outs,
        scratch_shapes=scratch,
        compiler_params=pltpu.CompilerParams(collective_id=0, has_side_effects=True, vmem_limit_bytes=VMEM_LIMIT),
        name="stack",
    )(*ins)


def solution(mesh):
    def step(x, dy, wg, wu, wd):
        dx, *out = call(x[0], dy[0], wg, wu, wd, wg.shape[2] // CHUNK)[6:]
        return dx[None], *out

    states, cut = P(("rep", "r", "s"), None, None), P(None, "s", None)
    return jax.shard_map(
        step,
        mesh=mesh,
        in_specs=(states, states) + (cut,) * 3,
        out_specs=(states,) + (P("rep", "s", None),) * 3,
        check_vma=False,
    )
```

```python
import functools

import jax
import jax.numpy as jnp
from jax import lax
from jax.experimental import pallas as pl
from jax.experimental.pallas import tpu as pltpu
from jax.sharding import PartitionSpec as P

RING = 4
BLOCK = 128
CHUNK = RING * BLOCK
BOTH = 2 * CHUNK
HALF = BLOCK // 2
PART = HALF // RING
VMEM_LIMIT = 66_900_000
SIDES = (1, 3)
OTHERS = (1, 2, 3)
ALL = (0, 1, 2, 3)
KINDS = (0, 1)
WIDE, DOWN = (0,), (1,)
f32, bf16 = jnp.float32, jnp.bfloat16


def dot(a, b):
    return jnp.dot(a, b, preferred_element_type=f32)


def dot_nt(a, b):
    return lax.dot_general(a, b, (((1,), (1,)), ((), ())), preferred_element_type=f32)


def dot_tn(a, b):
    return lax.dot_general(a, b, (((0,), (0,)), ((), ())), preferred_element_type=f32)


def rows_at(start, size, unit=None):
    return pl.ds(pl.multiple_of(start, size if unit is None else unit), size)


def add_up(*terms):
    total = terms[0].astype(f32)
    for term in terms[1:]:
        total = total + term.astype(f32)
    return total.astype(bf16)


def scale_of(wide):
    return lax.rsqrt(jnp.mean(wide**2, -1, keepdims=True) + 1e-6)


def normed(h):
    wide = h.astype(f32)
    return (wide * scale_of(wide)).astype(bf16)


def on(cond):
    return pl.when(cond)


class Place:
    def __init__(self):
        r, s = lax.axis_index("r"), lax.axis_index("s")
        self.y, self.z, self.x, self.c = r // RING, lax.rem(r, RING), s // 2, lax.rem(s, 2)

    def at(self, dy=0, dz=0, dx=0, dc=0):
        y, z, x = (lax.rem(v + d, RING) for v, d in ((self.y, dy), (self.z, dz), (self.x, dx)))
        return {"r": y * RING + z, "s": x * 2 + lax.rem(self.c + dc, 2)}

    def along(self, first, step, dc=0):
        return self.at(dy=first * step, dz=(1 - first) * step, dc=dc)


def send(src, dst, send_sem, recv_sem, device):
    pltpu.make_async_remote_copy(
        src_ref=src, dst_ref=dst, send_sem=send_sem, recv_sem=recv_sem, device_id=device, device_id_type=pl.DeviceIdType.MESH
    ).start()


def drain(ref, sem):
    pltpu.make_async_copy(ref, ref, sem).wait()


def meet(devices):
    barrier = pltpu.get_barrier_semaphore()
    for device in devices:
        pl.semaphore_signal(barrier, inc=1, device_id=device, device_id_type=pl.DeviceIdType.MESH)
    pl.semaphore_wait(barrier, len(devices))


class Gather:
    def __init__(self, place, chunks, wg, wu, wd, lent, full_gu, full_d, send_sem, recv_sem):
        self.p, self.chunks = place, chunks
        self.few = chunks // 2
        self.many = chunks - self.few
        self.wg, self.wu, self.wd, self.lent, self.gu, self.d = wg, wu, wd, lent, full_gu, full_d
        self.ss, self.rs = send_sem, recv_sem
        self.rows = wg.shape[1]
        self.total = wg.shape[0] * chunks

    def lend(self, sem):
        for l in range(2):
            for i in range(self.few):
                send(self.wd.at[l, pl.ds((2 * i + 1) * HALF, HALF), :], self.lent.at[l, i], sem.at[0], sem.at[1], self.p.at(dc=1))

    def settle_lend(self, sem):
        for i in range(2):
            drain(self.lent, sem.at[i])

    def with_down(self, n, use):
        l, k = n // self.chunks, lax.rem(n, self.chunks)
        c = self.p.c
        first = c * self.few
        owned = (k >= first) & (k < first + self.many)
        start = 2 * (k - first) * HALF

        @on(owned)
        def _():
            use(self.wd.at[l, rows_at(start, HALF), :])

        @on(jnp.logical_not(owned))
        def _():
            use(self.lent.at[l, k - (1 - c) * self.many])

    def of(self, n):
        k = lax.rem(n, self.chunks)
        first = self.p.c
        quarter = first * self.p.y + (1 - first) * self.p.z
        return n // self.chunks, k, first, quarter

    def sems(self, step, n):
        return self.ss.at[step, lax.rem(n, 2)], self.rs.at[step, lax.rem(n, 2)]

    def own_columns(self, j, k):
        return rows_at((j * self.chunks + k) * BLOCK, BLOCK)

    def piece(self, which, n, slots, quarter, part=None):
        share = 1 if part is None else 2
        offset = 0 if part is None else part
        if which == "d":
            size = PART // share
            return self.d.at[n, slots, self.p.c, rows_at(quarter * PART + offset * size, size), :]
        size = self.rows // share
        column = quarter * BLOCK + (CHUNK if which == "u" else 0)
        return self.gu.at[n, slots, self.p.c, pl.ds(offset * size, size), rows_at(column, BLOCK)]

    def settle(self, step, n, kinds, blocks, columns, rows):
        ss, rs = self.sems(step, n)
        refs = self.gu.at[0, pl.ds(0, blocks), 0, :, pl.ds(0, columns * BLOCK)], self.d.at[0, pl.ds(0, blocks), 0, pl.ds(0, rows), :]
        for i in kinds:
            for sems in (rs, ss):
                drain(refs[i], sems.at[i])

    def x1_wide(self, n):
        p = self.p
        l, k, _, _ = self.of(n)
        ss, rs = self.sems(0, n)
        for dx in SIDES:
            slot = RING - dx
            send(self.wg.at[l, :, self.own_columns(p.y, k)], self.piece("g", n, slot, p.y), ss.at[0], rs.at[0], p.at(dx=dx))
            send(self.wu.at[l, :, self.own_columns(p.z, k)], self.piece("u", n, slot, p.z), ss.at[0], rs.at[0], p.at(dx=dx))

    def x1_down(self, n):
        p = self.p
        _, _, _, q = self.of(n)
        ss, rs = self.sems(0, n)

        def use(ref):
            for dx in SIDES:
                send(ref.at[rows_at(q * PART, PART), :], self.piece("d", n, RING - dx, q), ss.at[1], rs.at[1], p.at(dx=dx))

        self.with_down(n, use)

    def x1(self, n):
        self.x1_wide(n)
        self.x1_down(n)

    def x2(self, n, kinds=KINDS):
        p = self.p
        _, _, _, q = self.of(n)
        self.settle(0, n, kinds, 1, 4, 2 * PART)
        ss, rs = self.sems(1, n)
        for part, to in enumerate(SIDES):
            for which, quarter, i in (("g", p.y, 0), ("u", p.z, 0), ("d", q, 1)):
                if i in kinds:
                    src, dst = (self.piece(which, n, slot, quarter, part) for slot in (RING - to, 2))
                    send(src, dst, ss.at[i], rs.at[i], p.at(dx=to))

    def round(self, n, kinds, step):
        p = self.p
        _, _, first, q = self.of(n)
        pieces = (("g", p.y, p.at(dy=step), 0), ("u", p.z, p.at(dz=step), 0), ("d", q, p.along(first, step), 1))
        return [piece for piece in pieces if piece[-1] in kinds]

    def yz1(self, n, kinds=KINDS):
        p = self.p
        self.settle(1, n, kinds, 1, 2, PART)
        ss, rs = self.sems(2, n)
        for step in SIDES:
            for which, quarter, to, i in self.round(n, kinds, step):
                ref = self.piece(which, n, pl.ds(1, 3), quarter)
                send(ref, ref, ss.at[i], rs.at[i], to)

    def yz2(self, n, kinds=KINDS):
        p = self.p
        self.settle(2, n, kinds, 3, 4, 2 * PART)
        ss, rs = self.sems(3, n)
        for part, step in enumerate(SIDES):
            for which, quarter, to, i in self.round(n, kinds, step):
                ref = self.piece(which, n, pl.ds(1, 3), lax.rem(quarter + RING - step, RING), part)
                send(ref, ref, ss.at[i], rs.at[i], to)

    def own(self, n, kinds, places, copy):
        l, k, _, _ = self.of(n)
        if 0 in kinds:
            for j in ALL:
                for i, w in enumerate((self.wg, self.wu)):
                    copy(w.at[l, :, self.own_columns(j, k)], places[0].at[:, pl.ds(i * CHUNK + j * BLOCK, BLOCK)], 0)
        if 1 in kinds:
            self.with_down(n, lambda ref: copy(ref, places[1], 1))

    def across(self, n, kinds=KINDS):
        c = self.p.c
        self.settle(3, n, kinds, 3, 2, PART)
        ss, rs = self.sems(4, n)
        to = self.p.at(dc=1)
        full = self.gu.at[n], self.d.at[n]
        self.own(n, kinds, [ref.at[0, c] for ref in full], lambda src, dst, i: send(src, dst, ss.at[i], rs.at[i], to))
        for i in kinds:
            ref = full[i].at[pl.ds(1, 3), c]
            send(ref, ref, ss.at[i], rs.at[i], to)

    def load(self, n, slot, into, sem, kinds=KINDS):
        p = self.p
        on(n < self.total)(lambda: self.settle(4, n, kinds, 4, 8, HALF))
        n = lax.rem(n, self.total)
        full = self.gu.at[n], self.d.at[n]
        sizes = self.rows, HALF
        place = lambda i, x, c: into[i].at[slot, rows_at((2 * x + c) * sizes[i], sizes[i], PART), :]
        start = lambda src, dst, i: pltpu.make_async_copy(src, dst, sem.at[slot, i]).start()
        self.own(n, kinds, [place(i, p.x, p.c) for i in KINDS], start)
        for i in kinds:
            start(full[i].at[0, 1 - p.c], place(i, p.x, 1 - p.c), i)
            for dx in OTHERS:
                for c in range(2):
                    start(full[i].at[dx, c], place(i, lax.rem(p.x + dx, RING), c), i)


def vmem(*shape, dtype=bf16):
    return pltpu.VMEM(shape, dtype)


def dma(*shape):
    return pltpu.SemaphoreType.DMA(shape)


class Reduce:
    def __init__(self, place, chunks, kind, own, out, bufs, sems):
        self.p, self.chunks, self.kind, self.own, self.out = place, chunks, kind, own, out
        self.pair_v, self.r1, self.s1, self.r2, self.s2, self.f, self.y, self.z, self.o = bufs
        self.pair_s, self.pair_r, self.s1_s, self.s1_r, self.s2_s, self.s2_r, self.y_s, self.y_r, self.z_s, self.z_r, self.o_s, self.o_r, self.l_sem, self.c_r = sems
        self.rows = self.f.shape[1]

    @staticmethod
    def scratch(kind, rows, d, chunks):
        block, axis = ([rows, CHUNK], 1) if kind < 2 else ([HALF, d], 0)

        def buf(lead, parts):
            shape = list(block)
            shape[axis] //= parts
            return vmem(*lead, *shape)

        r1, s1, r2, s2 = (buf(lead, parts) for parts in (2, 1) for lead in ((2, 2), (2,)))
        bufs = [buf((3, RING), 1), r1, s1, r2, s2, buf((2,), 1), buf((2, 3), RING), buf((2, RING), RING), buf((2,), RING)]
        sems = [dma(3)] * 2 + [dma(1), dma(2)] * 2 + [dma(2)] * 7 + [dma(2 * chunks)]
        return bufs, sems

    def part(self, i, parts):
        if self.kind < 2:
            return slice(None), rows_at(i * (CHUNK // parts), CHUNK // parts)
        return rows_at(i * (HALF // parts), HALF // parts), slice(None)

    def device_rows(self, x, c):
        return rows_at((2 * x + c) * self.rows, self.rows, PART)

    def pair(self, q):
        p = self.p
        slot, slot3 = lax.rem(q, 2), lax.rem(q, 3)
        for x in ALL:
            send(self.own.at[slot, self.device_rows(x, 1 - p.c), :], self.pair_v.at[slot3, x], self.pair_s.at[slot3], self.pair_r.at[slot3], p.at(dc=1))

    def terms(self, q, x, i, parts):
        rows, columns = self.part(i, parts)
        own = self.own.at[lax.rem(q, 2), self.device_rows(x, self.p.c), :]
        return own[rows, columns], self.pair_v.at[lax.rem(q, 3), x][rows, columns]

    def x1(self, q):
        p = self.p
        slot, slot3 = lax.rem(q, 2), lax.rem(q, 3)
        for sem in (self.pair_r, self.pair_s):
            drain(self.pair_v.at[slot3], sem.at[slot3])
        for i in range(2):
            self.s1[i] = add_up(*self.terms(q, lax.rem(p.x + 2, RING), i, 2))
        for i, dx in enumerate(SIDES):
            send(self.s1.at[i], self.r1.at[slot, i], self.s1_s.at[0], self.s1_r.at[slot], p.at(dx=dx))

    def x2(self, q):
        p = self.p
        slot = lax.rem(q, 2)
        drain(self.r1.at[slot], self.s1_r.at[slot])
        drain(self.s1, self.s1_s.at[0])
        for i, dx in enumerate(SIDES):
            for j in range(2):
                more = (self.r1[slot, i],) if i == j else ()
                self.s2.at[i][self.part(j, 2)] = add_up(*self.terms(q, lax.rem(p.x + dx, RING), j, 2), *more)
            send(self.s2.at[i], self.r2.at[slot, i], self.s2_s.at[0], self.s2_r.at[slot], p.at(dx=dx))

    def of(self, q):
        p = self.p
        first = (1, 0, p.c)[self.kind]
        return first, first * p.y + (1 - first) * p.z, first * p.z + (1 - first) * p.y

    def yz1(self, q):
        p = self.p
        slot = lax.rem(q, 2)
        drain(self.r2.at[slot], self.s2_r.at[slot])
        drain(self.s2, self.s2_s.at[0])
        self.f[slot] = add_up(*self.terms(q, p.x, 0, 1), *(self.r2[slot, i] for i in range(2)))
        first, along, _ = self.of(q)
        for i, step in enumerate(OTHERS):
            src = self.f.at[(slot, *self.part(lax.rem(along + step, RING), RING))]
            send(src, self.y.at[slot, i], self.y_s.at[slot], self.y_r.at[slot], p.along(first, step))

    def yz2(self, q):
        p = self.p
        slot = lax.rem(q, 2)
        for sem in (self.y_r, self.y_s):
            drain(self.y.at[slot], sem.at[slot])
        first, along, over = self.of(q)
        self.z[slot, over] = add_up(self.f.at[slot][self.part(along, RING)], *(self.y[slot, i] for i in range(3)))
        for step in OTHERS:
            send(self.z.at[slot, over], self.z.at[slot, over], self.z_s.at[slot], self.z_r.at[slot], p.along(1 - first, step))

    def place_of(self, q):
        p = self.p
        l, k = 1 - q // self.chunks, lax.rem(q, self.chunks)
        _, along, _ = self.of(q)
        if self.kind < 2:
            return self.out.at[l, :, rows_at((along * self.chunks + k) * BLOCK, BLOCK)], None
        rows = self.chunks * HALF
        row = k * BLOCK + p.c * HALF + along * PART
        return self.out.at[l, rows_at(lax.rem(row, rows), PART), :], row // rows == p.c

    def lends(self, q):
        row = lax.rem(q, self.chunks) * BLOCK + (1 - self.p.c) * HALF
        return row // (self.chunks * HALF) == self.p.c

    def yz3(self, q):
        p = self.p
        slot = lax.rem(q, 2)
        for sem in (self.z_r, self.z_s):
            drain(self.z.at[slot, pl.ds(0, 3)], sem.at[slot])
        self.o[slot] = add_up(*(self.z[slot, i] for i in ALL))
        first, _, _ = self.of(q)
        out, owned = self.place_of(q)

        def spread():
            pltpu.make_async_copy(self.o.at[slot], out, self.l_sem.at[slot]).start()
            for step in OTHERS:
                send(self.o.at[slot], out, self.o_s.at[slot], self.o_r.at[slot], p.along(first, step))

        if owned is None:
            spread()
            return
        on(owned)(spread)

        @on(jnp.logical_not(owned))
        def _():
            for step in ALL:
                send(self.o.at[slot], out, self.o_s.at[slot], self.c_r.at[q], p.along(first, step, dc=1))

    def finish(self, q):
        slot = lax.rem(q, 2)
        _, owned = self.place_of(q)

        def settle():
            for sem in (self.o_r, self.o_s):
                drain(self.y.at[slot], sem.at[slot])
            drain(self.o.at[slot], self.l_sem.at[slot])

        if owned is None:
            settle()
            return
        on(owned)(settle)

        @on(jnp.logical_not(owned))
        def _():
            drain(self.z.at[slot], self.o_s.at[slot])

        @on(self.lends(q))
        def _():
            drain(self.z.at[slot], self.c_r.at[q])


def kernel(chunks, x_ref, dy_ref, wg, wu, wd, full_gu, full_d, lent, kept, h_ref, spill, dx_ref, out_g, out_u, out_d, *scratch):
    a_v, dy_v, da_v, gu_v, d_v, dgu_v, act_v, kept_v, own, (ss, rs, ld_sem, kept_sem, io_sem, lend_sem), reduces = scratch
    p = Place()
    meet([p.at(dc=1)] + [p.at(dx=side) for side in SIDES] + [p.at(**{axis: step}, dc=dc) for axis in ("dy", "dz") for step in OTHERS for dc in range(2)])
    tokens, d = a_v.shape
    half = tokens // 2
    small = min(BLOCK, half)
    g = Gather(p, chunks, wg, wu, wd, lent, full_gu, full_d, ss, rs)
    parts = [Reduce(p, chunks, kind, own[kind], (out_g, out_u, out_d)[kind], *reduces[kind]) for kind in (2, 0, 1)]
    total = 2 * chunks

    def tiles(start, stop, count, use):
        steps = tokens // small

        @pl.loop(start * steps // count, stop * steps // count)
        def _(i):
            use(rows_at(i * small, small))

    x_copy = pltpu.make_async_copy(x_ref, dy_v, io_sem.at[0])
    x_copy.start()
    g.lend(lend_sem)
    g.x1_wide(0)
    x_copy.wait()

    def first_norm(t):
        a_v[t, :] = normed(dy_v[t, :])
        da_v[t, :] = jnp.zeros((small, d), f32)

    into = (gu_v, d_v)
    tiles(0, 1, 4, first_norm)
    g.settle_lend(lend_sem)
    g.x1_down(0)
    tiles(1, 3, 4, first_norm)
    g.x2(0, WIDE)
    g.x2(0, DOWN)
    g.x1(1)
    tiles(3, 4, 4, first_norm)
    g.yz1(0, WIDE)
    g.yz1(0, DOWN)
    g.x2(1)
    g.x1(2)
    g.yz2(0, WIDE)
    g.yz2(0, DOWN)
    g.yz1(1)
    g.x2(2)
    g.x1(3)
    g.across(0, WIDE)
    g.across(0, DOWN)
    g.yz1(2)
    g.load(0, 0, into, ld_sem, WIDE)
    g.load(0, 0, into, ld_sem, DOWN)
    g.yz2(1)
    g.x2(3)
    g.x1(4)

    def loaded(n, i):
        drain(into[i].at[lax.rem(n, 2)], ld_sem.at[lax.rem(n, 2), i])

    def gather_on(n):
        for i, step in enumerate((g.across, g.yz2, g.yz1, g.x2, g.x1)):
            on(n + i + 1 < total)(functools.partial(step, n + i + 1))

    def forward_part(k, i):
        slot = lax.rem(k, 2)
        t = rows_at(i * half, half)

        @on(k > 0)
        def _():
            drain(kept_v.at[i], kept_sem.at[i])

        kept_v[i] = dot(a_v[t, :], gu_v[slot])
        pltpu.make_async_copy(kept_v.at[i], kept.at[k, t, :], kept_sem.at[i]).start()
        gate, up = kept_v[i, :, :CHUNK], kept_v[i, :, CHUNK:]
        act = (jax.nn.silu(gate) * up).astype(bf16)
        on(i == 0)(lambda: loaded(k, 1))
        da_v[t, :] += dot(act, d_v[slot])

    @pl.loop(0, chunks)
    def _(k):
        on(k > 0)(lambda: gather_on(k))
        loaded(k, 0)

        @pl.loop(0, 2)
        def _(i):
            @on(i == 1)
            def _():
                on(k == 0)(lambda: gather_on(k))
                on(k > 0)(lambda: g.load(k + 1, lax.rem(k + 1, 2), into, ld_sem))

            forward_part(k, i)

        on(k == 0)(lambda: g.load(k + 1, lax.rem(k + 1, 2), into, ld_sem))

    def between(t):
        h = add_up(dy_v[t, :], da_v[t, :].astype(bf16))
        dy_v[t, :] = h
        a_v[t, :] = normed(h)
        da_v[t, :] = jnp.zeros((small, d), f32)
        pltpu.make_async_copy(dy_v.at[t, :], h_ref.at[t, :], io_sem.at[1]).start()

    tiles(0, 1, 1, between)
    drain(dy_v, io_sem.at[1])
    dy_copy = pltpu.make_async_copy(dy_ref, dy_v, io_sem.at[0])
    dy_copy.start()
    for i in range(2):
        drain(kept_v.at[i], kept_sem.at[i])

    def each(step, q):
        for part in parts:
            getattr(part, step)(q)

    def fetch(ref):
        return pltpu.make_async_copy(ref, a_v, io_sem.at[0])

    def keep(t):
        b = lax.rem(t, 2)
        return pltpu.make_async_copy(kept.at[t // 2, rows_at(b * half, half), :], kept_v.at[b], kept_sem.at[b])

    def through_norm(start, stop, then):
        def use(t):
            wide = a_v[t, :].astype(f32)
            scale = scale_of(wide)
            hat = wide * scale
            da = da_v[t, :].astype(bf16).astype(f32)
            back = scale * (da - hat * jnp.mean(da * hat, -1, keepdims=True))
            dy_v[t, :] = add_up(dy_v[t, :], back.astype(bf16))
            da_v[t, :] = jnp.zeros((small, d), f32)
            then(t)

        tiles(start, stop, 2, use)

    def through_gate(t, gate, up, slot):
        dact = dot_nt(dy_v[t, :], d_v[slot]).astype(bf16).astype(f32)
        sig = jax.nn.sigmoid(gate)
        silu = gate * sig
        act_v[t, :] = (silu * up).astype(bf16)
        dgu_v[t, :CHUNK] = (dact * up * (sig * (1 + gate * (1 - sig)))).astype(bf16)
        dgu_v[t, CHUNK:] = (dact * silu).astype(bf16)

    def da_tile(t, slot):
        da_v[t, :] += dot_nt(dgu_v[t, :], gu_v[slot])

    def gate_part(q, slot, i):
        k = lax.rem(q, chunks)

        def layer1(joined):
            t = rows_at(i * half, half)
            if joined:
                da_tile(t, 1 - slot)
            gu = dot(a_v[t, :], gu_v[slot])
            if not joined:
                on(i == 0)(dy_copy.wait)
            through_gate(t, gu[:, :CHUNK], gu[:, CHUNK:], slot)

        def layer0(joined):
            n = (q - chunks) * 2 + i
            keep(n).wait()
            t = rows_at(i * half, half)
            if joined:
                da_tile(t, 1 - slot)
            through_gate(t, kept_v[i, :, :CHUNK], kept_v[i, :, CHUNK:], slot)

            @on(n + 2 < 2 * chunks)
            def _():
                keep(n + 2).start()

        joins = (k > 0) & (q != total - 1)
        for joined in (False, True):
            on((q < chunks) & (joins == joined))(functools.partial(layer1, joined))
            on((q >= chunks) & (q < total) & (joins == joined))(functools.partial(layer0, joined))

    away_copy = pltpu.make_async_copy(dgu_v, spill, io_sem.at[1])

    def back_copy(i):
        t = rows_at(i * half, half)
        return pltpu.make_async_copy(spill.at[t, :], dgu_v.at[t, :], kept_sem.at[i])

    @pl.loop(0, total + 4)
    def _(q):
        slot, side = lax.rem(q, 2), lax.rem(q + chunks, 2)
        busy = q < total
        ahead = chunks + q
        one = (q >= 1) & (q <= total)
        two = (q >= 2) & (q <= total + 1)
        three = (q >= 3) & (q <= total + 2)

        @on(three & (q != total + 1))
        def _():
            each("yz2", q - 3)

        @on(q >= 4)
        def _():
            each("finish", q - 4)

        @pl.loop(0, jnp.where(q == total, 4, jnp.where(q == chunks, 2, 0)))
        def _(i):
            j = lax.rem(i, 2)
            on((q == total) & (i == 1))(lambda: each("x1", q - 1))

            @on(i == 3)
            def _():
                each("yz3", q - 3)
                each("yz1", q - 2)
                each("x2", q - 1)

            on(i >= 2)(back_copy(j).wait)
            da_tile(rows_at(j * half, half), jnp.where(i < 2, 1 - side, side))
            on((q == total) & (i < 2))(back_copy(j).start)

        on(q == total - 1)(away_copy.wait)

        @on(q == chunks)
        def _():
            fetch(h_ref).wait()

            def then(t):
                pltpu.make_async_copy(x_ref.at[t, :], a_v.at[t, :], io_sem.at[0]).start()

            through_norm(0, 2, then)
            fetch(x_ref).wait()

            def again(t):
                a_v[t, :] = normed(a_v[t, :])

            tiles(0, 1, 1, again)

        gather_on(ahead)

        @on(busy)
        def _():
            loaded(ahead, 0)
            loaded(ahead, 1)

        @pl.loop(0, 2)
        def _(i):
            @on((q >= 1) & (q < total) & (i == 1))
            def _():
                each("x1", q - 1)

            gate_part(q, side, i)

        on(q == total - 2)(away_copy.start)

        @on(three & (q != total))
        def _():
            each("yz3", q - 3)

        @on(two & (q != total))
        def _():
            each("yz1", q - 2)

        @on(q + 1 < total)
        def _():
            g.load(ahead + 1, 1 - side, into, ld_sem)

        @on(busy)
        def _():
            own[2][slot] = dot_tn(act_v[...], dy_v[...]).astype(bf16)
            parts[0].pair(q)

        @on(q == total)
        def _():
            fetch(x_ref).wait()
            through_norm(0, 1, lambda t: None)
            each("yz2", q - 2)

        @on(one & (q != total))
        def _():
            each("x2", q - 1)

        @on(busy)
        def _():
            both = dot_tn(a_v[...], dgu_v[...]).astype(bf16)
            own[0][slot] = both[:, :CHUNK]
            own[1][slot] = both[:, CHUNK:]
            for part in parts[1:]:
                part.pair(q)

        @on(q == total)
        def _():
            through_norm(1, 2, lambda t: None)
            pltpu.make_async_copy(dy_v, dx_ref, io_sem.at[0]).start()

        @on(q == chunks - 1)
        def _():
            fetch(h_ref).start()
            keep(0).start()
            keep(1).start()

        @on(q == total - 1)
        def _():
            fetch(x_ref).start()

    pltpu.make_async_copy(dy_v, dx_ref, io_sem.at[0]).wait()


def call(x, dy, wg, wu, wd, chunks):
    tokens, d = x.shape
    layers, rows, _ = wg.shape
    n = layers * chunks
    shapes = [(n, RING, 2, rows, BOTH), (n, RING, 2, HALF, d), (layers, chunks // 2, HALF, d), (chunks, tokens, BOTH), x.shape, (tokens, BOTH), x.shape, wg.shape, wu.shape, wd.shape]
    outs = [jax.ShapeDtypeStruct(shape, f32 if shape == (chunks, tokens, BOTH) else bf16) for shape in shapes]
    scratch = [vmem(tokens, d)] * 2 + [vmem(tokens, d, dtype=f32), vmem(2, d, BOTH), vmem(2, CHUNK, d)]
    scratch += [vmem(tokens, BOTH), vmem(tokens, CHUNK), vmem(2, tokens // 2, BOTH, dtype=f32)]
    scratch += [[vmem(2, d, CHUNK)] * 2 + [vmem(2, CHUNK, d)]]
    scratch += [[dma(5, 2, 2)] * 2 + [dma(2, 2)] + [dma(2)] * 3]
    scratch += [[Reduce.scratch(kind, rows, d, chunks) for kind in range(3)]]
    any_ = pl.BlockSpec(memory_space=pl.ANY)
    ins = (x, dy, wg, wu, wd)
    return pl.pallas_call(
        functools.partial(kernel, chunks),
        in_specs=[any_] * len(ins),
        out_specs=[any_] * len(outs),
        out_shape=outs,
        scratch_shapes=scratch,
        compiler_params=pltpu.CompilerParams(collective_id=0, has_side_effects=True, vmem_limit_bytes=VMEM_LIMIT),
        name="stack",
    )(*ins)


def hand_on_kernel(cuts, *refs):
    count = len(cuts)
    ins, outs, bufs = (refs[i * count : (i + 1) * count] for i in range(3))
    in_sem, out_sem = refs[3 * count :]
    jobs = []
    for src, dst, buf, cut in zip(ins, outs, bufs, cuts):
        size = src.shape[0] // cut
        for j in range(cut):
            t = pl.ds(j * size, size)
            i = len(jobs)
            jobs.append((pltpu.make_async_copy(src.at[t], buf.at[t], in_sem.at[i]), pltpu.make_async_copy(buf.at[t], dst.at[t], out_sem.at[i])))
    for come, _ in jobs:
        come.start()
    for come, go in jobs:
        come.wait()
        go.start()
    for _, go in jobs:
        go.wait()


def hand_on(*arrays):
    cuts = [8 if v.ndim == 2 else v.shape[0] for v in arrays]
    any_ = pl.BlockSpec(memory_space=pl.ANY)
    return pl.pallas_call(
        functools.partial(hand_on_kernel, cuts),
        in_specs=[any_] * len(arrays),
        out_specs=[any_] * len(arrays),
        out_shape=[jax.ShapeDtypeStruct(v.shape, bf16) for v in arrays],
        scratch_shapes=[vmem(*v.shape) for v in arrays] + [dma(sum(cuts))] * 2,
        name="hand_on",
    )(*arrays)


def solution(mesh):
    def step(x, dy, wg, wu, wd):
        dx, *out = hand_on(*call(x[0], dy[0], wg, wu, wd, wg.shape[2] // CHUNK)[6:])
        return dx[None], *out

    states, cut = P(("rep", "r", "s"), None, None), P(None, "s", None)
    return jax.shard_map(
        step,
        mesh=mesh,
        in_specs=(states, states) + (cut,) * 3,
        out_specs=(states,) + (P("rep", "s", None),) * 3,
        check_vma=False,
    )
```

```python
import functools

import jax
import jax.numpy as jnp
from jax import lax
from jax.experimental import pallas as pl
from jax.experimental.pallas import tpu as pltpu
from jax.sharding import PartitionSpec as P

RING = 4
BLOCK = 128
CHUNK = RING * BLOCK
BOTH = 2 * CHUNK
HALF = BLOCK // 2
PART = HALF // RING
VMEM_LIMIT = 66_900_000
SIDES = (1, 3)
OTHERS = (1, 2, 3)
ALL = (0, 1, 2, 3)
KINDS = (0, 1)
WIDE, DOWN = (0,), (1,)
f32, bf16 = jnp.float32, jnp.bfloat16


def dot(a, b):
    return jnp.dot(a, b, preferred_element_type=f32)


def dot_nt(a, b):
    return lax.dot_general(a, b, (((1,), (1,)), ((), ())), preferred_element_type=f32)


def dot_tn(a, b):
    return lax.dot_general(a, b, (((0,), (0,)), ((), ())), preferred_element_type=f32)


def rows_at(start, size, unit=None):
    return pl.ds(pl.multiple_of(start, size if unit is None else unit), size)


def add_up(*terms):
    total = terms[0].astype(f32)
    for term in terms[1:]:
        total = total + term.astype(f32)
    return total.astype(bf16)


def scale_of(wide):
    return lax.rsqrt(jnp.mean(wide**2, -1, keepdims=True) + 1e-6)


def normed(h):
    wide = h.astype(f32)
    return (wide * scale_of(wide)).astype(bf16)


def on(cond):
    return pl.when(cond)


class Place:
    def __init__(self):
        r, s = lax.axis_index("r"), lax.axis_index("s")
        self.y, self.z, self.x, self.c = r // RING, lax.rem(r, RING), s // 2, lax.rem(s, 2)

    def at(self, dy=0, dz=0, dx=0, dc=0):
        y, z, x = (lax.rem(v + d, RING) for v, d in ((self.y, dy), (self.z, dz), (self.x, dx)))
        return {"r": y * RING + z, "s": x * 2 + lax.rem(self.c + dc, 2)}

    def along(self, first, step, dc=0):
        return self.at(dy=first * step, dz=(1 - first) * step, dc=dc)


def send(src, dst, send_sem, recv_sem, device):
    pltpu.make_async_remote_copy(
        src_ref=src, dst_ref=dst, send_sem=send_sem, recv_sem=recv_sem, device_id=device, device_id_type=pl.DeviceIdType.MESH
    ).start()


def drain(ref, sem):
    pltpu.make_async_copy(ref, ref, sem).wait()


def meet(devices):
    barrier = pltpu.get_barrier_semaphore()
    for device in devices:
        pl.semaphore_signal(barrier, inc=1, device_id=device, device_id_type=pl.DeviceIdType.MESH)
    pl.semaphore_wait(barrier, len(devices))


class Gather:
    def __init__(self, place, chunks, wg, wu, wd, lent, full_gu, full_d, send_sem, recv_sem):
        self.p, self.chunks = place, chunks
        self.few = chunks // 2
        self.many = chunks - self.few
        self.wg, self.wu, self.wd, self.lent, self.gu, self.d = wg, wu, wd, lent, full_gu, full_d
        self.ss, self.rs = send_sem, recv_sem
        self.rows = wg.shape[1]
        self.total = wg.shape[0] * chunks

    def lend(self, sem):
        for l in range(2):
            for i in range(self.few):
                send(self.wd.at[l, pl.ds((2 * i + 1) * HALF, HALF), :], self.lent.at[l, i], sem.at[0], sem.at[1], self.p.at(dc=1))

    def settle_lend(self, sem):
        for i in range(2):
            drain(self.lent, sem.at[i])

    def with_down(self, n, use):
        l, k = n // self.chunks, lax.rem(n, self.chunks)
        c = self.p.c
        first = c * self.few
        owned = (k >= first) & (k < first + self.many)
        start = 2 * (k - first) * HALF

        @on(owned)
        def _():
            use(self.wd.at[l, rows_at(start, HALF), :])

        @on(jnp.logical_not(owned))
        def _():
            use(self.lent.at[l, k - (1 - c) * self.many])

    def of(self, n):
        k = lax.rem(n, self.chunks)
        first = self.p.c
        quarter = first * self.p.y + (1 - first) * self.p.z
        return n // self.chunks, k, first, quarter

    def sems(self, step, n):
        return self.ss.at[step, lax.rem(n, 2)], self.rs.at[step, lax.rem(n, 2)]

    def own_columns(self, j, k):
        return rows_at((j * self.chunks + k) * BLOCK, BLOCK)

    def piece(self, which, n, slots, quarter, part=None):
        share = 1 if part is None else 2
        offset = 0 if part is None else part
        if which == "d":
            size = PART // share
            return self.d.at[n, slots, self.p.c, rows_at(quarter * PART + offset * size, size), :]
        size = self.rows // share
        column = quarter * BLOCK + (CHUNK if which == "u" else 0)
        return self.gu.at[n, slots, self.p.c, pl.ds(offset * size, size), rows_at(column, BLOCK)]

    def settle(self, step, n, kinds, blocks, columns, rows):
        ss, rs = self.sems(step, n)
        refs = self.gu.at[0, pl.ds(0, blocks), 0, :, pl.ds(0, columns * BLOCK)], self.d.at[0, pl.ds(0, blocks), 0, pl.ds(0, rows), :]
        for i in kinds:
            for sems in (rs, ss):
                drain(refs[i], sems.at[i])

    def x1_wide(self, n):
        p = self.p
        l, k, _, _ = self.of(n)
        ss, rs = self.sems(0, n)
        for dx in SIDES:
            slot = RING - dx
            send(self.wg.at[l, :, self.own_columns(p.y, k)], self.piece("g", n, slot, p.y), ss.at[0], rs.at[0], p.at(dx=dx))
            send(self.wu.at[l, :, self.own_columns(p.z, k)], self.piece("u", n, slot, p.z), ss.at[0], rs.at[0], p.at(dx=dx))

    def x1_down(self, n):
        p = self.p
        _, _, _, q = self.of(n)
        ss, rs = self.sems(0, n)

        def use(ref):
            for dx in SIDES:
                send(ref.at[rows_at(q * PART, PART), :], self.piece("d", n, RING - dx, q), ss.at[1], rs.at[1], p.at(dx=dx))

        self.with_down(n, use)

    def x1(self, n):
        self.x1_wide(n)
        self.x1_down(n)

    def x2(self, n, kinds=KINDS):
        p = self.p
        _, _, _, q = self.of(n)
        self.settle(0, n, kinds, 1, 4, 2 * PART)
        ss, rs = self.sems(1, n)
        for part, to in enumerate(SIDES):
            for which, quarter, i in (("g", p.y, 0), ("u", p.z, 0), ("d", q, 1)):
                if i in kinds:
                    src, dst = (self.piece(which, n, slot, quarter, part) for slot in (RING - to, 2))
                    send(src, dst, ss.at[i], rs.at[i], p.at(dx=to))

    def round(self, n, kinds, step):
        p = self.p
        _, _, first, q = self.of(n)
        pieces = (("g", p.y, p.at(dy=step), 0), ("u", p.z, p.at(dz=step), 0), ("d", q, p.along(first, step), 1))
        return [piece for piece in pieces if piece[-1] in kinds]

    def yz1(self, n, kinds=KINDS):
        p = self.p
        self.settle(1, n, kinds, 1, 2, PART)
        ss, rs = self.sems(2, n)
        for step in SIDES:
            for which, quarter, to, i in self.round(n, kinds, step):
                ref = self.piece(which, n, pl.ds(1, 3), quarter)
                send(ref, ref, ss.at[i], rs.at[i], to)

    def yz2(self, n, kinds=KINDS):
        p = self.p
        self.settle(2, n, kinds, 3, 4, 2 * PART)
        ss, rs = self.sems(3, n)
        for part, step in enumerate(SIDES):
            for which, quarter, to, i in self.round(n, kinds, step):
                ref = self.piece(which, n, pl.ds(1, 3), lax.rem(quarter + RING - step, RING), part)
                send(ref, ref, ss.at[i], rs.at[i], to)

    def own(self, n, kinds, places, copy):
        l, k, _, _ = self.of(n)
        if 0 in kinds:
            for j in ALL:
                for i, w in enumerate((self.wg, self.wu)):
                    copy(w.at[l, :, self.own_columns(j, k)], places[0].at[:, pl.ds(i * CHUNK + j * BLOCK, BLOCK)], 0)
        if 1 in kinds:
            self.with_down(n, lambda ref: copy(ref, places[1], 1))

    def across(self, n, kinds=KINDS):
        c = self.p.c
        self.settle(3, n, kinds, 3, 2, PART)
        ss, rs = self.sems(4, n)
        to = self.p.at(dc=1)
        full = self.gu.at[n], self.d.at[n]
        self.own(n, kinds, [ref.at[0, c] for ref in full], lambda src, dst, i: send(src, dst, ss.at[i], rs.at[i], to))
        for i in kinds:
            ref = full[i].at[pl.ds(1, 3), c]
            send(ref, ref, ss.at[i], rs.at[i], to)

    def load(self, n, slot, into, sem, kinds=KINDS):
        p = self.p
        on(n < self.total)(lambda: self.settle(4, n, kinds, 4, 8, HALF))
        n = lax.rem(n, self.total)
        full = self.gu.at[n], self.d.at[n]
        sizes = self.rows, HALF
        place = lambda i, x, c: into[i].at[slot, rows_at((2 * x + c) * sizes[i], sizes[i], PART), :]
        start = lambda src, dst, i: pltpu.make_async_copy(src, dst, sem.at[slot, i]).start()
        self.own(n, kinds, [place(i, p.x, p.c) for i in KINDS], start)
        for i in kinds:
            start(full[i].at[0, 1 - p.c], place(i, p.x, 1 - p.c), i)
            for dx in OTHERS:
                for c in range(2):
                    start(full[i].at[dx, c], place(i, lax.rem(p.x + dx, RING), c), i)


def vmem(*shape, dtype=bf16):
    return pltpu.VMEM(shape, dtype)


def dma(*shape):
    return pltpu.SemaphoreType.DMA(shape)


class Reduce:
    def __init__(self, place, chunks, kind, own, out, bufs, sems):
        self.p, self.chunks, self.kind, self.own, self.out = place, chunks, kind, own, out
        self.pair_v, self.r1, self.s1, self.r2, self.s2, self.f, self.y, self.z, self.o = bufs
        self.pair_s, self.pair_r, self.s1_s, self.s1_r, self.s2_s, self.s2_r, self.y_s, self.y_r, self.z_s, self.z_r, self.o_s, self.o_r, self.l_sem, self.c_r = sems
        self.rows = self.f.shape[1]

    @staticmethod
    def scratch(kind, rows, d, chunks):
        block, axis = ([rows, CHUNK], 1) if kind < 2 else ([HALF, d], 0)

        def buf(lead, parts):
            shape = list(block)
            shape[axis] //= parts
            return vmem(*lead, *shape)

        r1, s1, r2, s2 = (buf(lead, parts) for parts in (2, 1) for lead in ((2, 2), (2,)))
        bufs = [buf((3, RING), 1), r1, s1, r2, s2, buf((2,), 1), buf((2, 3), RING), buf((2, RING), RING), buf((2,), RING)]
        sems = [dma(3)] * 2 + [dma(1), dma(2)] * 2 + [dma(2)] * 7 + [dma(2 * chunks)]
        return bufs, sems

    def part(self, i, parts):
        if self.kind < 2:
            return slice(None), rows_at(i * (CHUNK // parts), CHUNK // parts)
        return rows_at(i * (HALF // parts), HALF // parts), slice(None)

    def device_rows(self, x, c):
        return rows_at((2 * x + c) * self.rows, self.rows, PART)

    def pair(self, q):
        p = self.p
        slot, slot3 = lax.rem(q, 2), lax.rem(q, 3)
        for x in ALL:
            send(self.own.at[slot, self.device_rows(x, 1 - p.c), :], self.pair_v.at[slot3, x], self.pair_s.at[slot3], self.pair_r.at[slot3], p.at(dc=1))

    def terms(self, q, x, i, parts):
        rows, columns = self.part(i, parts)
        own = self.own.at[lax.rem(q, 2), self.device_rows(x, self.p.c), :]
        return own[rows, columns], self.pair_v.at[lax.rem(q, 3), x][rows, columns]

    def x1(self, q):
        p = self.p
        slot, slot3 = lax.rem(q, 2), lax.rem(q, 3)
        for sem in (self.pair_r, self.pair_s):
            drain(self.pair_v.at[slot3], sem.at[slot3])
        for i in range(2):
            self.s1[i] = add_up(*self.terms(q, lax.rem(p.x + 2, RING), i, 2))
        for i, dx in enumerate(SIDES):
            send(self.s1.at[i], self.r1.at[slot, i], self.s1_s.at[0], self.s1_r.at[slot], p.at(dx=dx))

    def x2(self, q):
        p = self.p
        slot = lax.rem(q, 2)
        drain(self.r1.at[slot], self.s1_r.at[slot])
        drain(self.s1, self.s1_s.at[0])
        for i, dx in enumerate(SIDES):
            for j in range(2):
                more = (self.r1[slot, i],) if i == j else ()
                self.s2.at[i][self.part(j, 2)] = add_up(*self.terms(q, lax.rem(p.x + dx, RING), j, 2), *more)
            send(self.s2.at[i], self.r2.at[slot, i], self.s2_s.at[0], self.s2_r.at[slot], p.at(dx=dx))

    def of(self, q):
        p = self.p
        first = (1, 0, p.c)[self.kind]
        return first, first * p.y + (1 - first) * p.z, first * p.z + (1 - first) * p.y

    def yz1(self, q):
        p = self.p
        slot = lax.rem(q, 2)
        drain(self.r2.at[slot], self.s2_r.at[slot])
        drain(self.s2, self.s2_s.at[0])
        self.f[slot] = add_up(*self.terms(q, p.x, 0, 1), *(self.r2[slot, i] for i in range(2)))
        first, along, _ = self.of(q)
        for i, step in enumerate(OTHERS):
            src = self.f.at[(slot, *self.part(lax.rem(along + step, RING), RING))]
            send(src, self.y.at[slot, i], self.y_s.at[slot], self.y_r.at[slot], p.along(first, step))

    def yz2(self, q):
        p = self.p
        slot = lax.rem(q, 2)
        for sem in (self.y_r, self.y_s):
            drain(self.y.at[slot], sem.at[slot])
        first, along, over = self.of(q)
        self.z[slot, over] = add_up(self.f.at[slot][self.part(along, RING)], *(self.y[slot, i] for i in range(3)))
        for step in OTHERS:
            send(self.z.at[slot, over], self.z.at[slot, over], self.z_s.at[slot], self.z_r.at[slot], p.along(1 - first, step))

    def place_of(self, q):
        p = self.p
        l, k = 1 - q // self.chunks, lax.rem(q, self.chunks)
        _, along, _ = self.of(q)
        if self.kind < 2:
            return self.out.at[l, :, rows_at((along * self.chunks + k) * BLOCK, BLOCK)], None
        rows = self.chunks * HALF
        row = k * BLOCK + p.c * HALF + along * PART
        return self.out.at[l, rows_at(lax.rem(row, rows), PART), :], row // rows == p.c

    def lends(self, q):
        row = lax.rem(q, self.chunks) * BLOCK + (1 - self.p.c) * HALF
        return row // (self.chunks * HALF) == self.p.c

    def yz3(self, q):
        p = self.p
        slot = lax.rem(q, 2)
        for sem in (self.z_r, self.z_s):
            drain(self.z.at[slot, pl.ds(0, 3)], sem.at[slot])
        self.o[slot] = add_up(*(self.z[slot, i] for i in ALL))
        first, _, _ = self.of(q)
        out, owned = self.place_of(q)

        def spread():
            pltpu.make_async_copy(self.o.at[slot], out, self.l_sem.at[slot]).start()
            for step in OTHERS:
                send(self.o.at[slot], out, self.o_s.at[slot], self.o_r.at[slot], p.along(first, step))

        if owned is None:
            spread()
            return
        on(owned)(spread)

        @on(jnp.logical_not(owned))
        def _():
            for step in ALL:
                send(self.o.at[slot], out, self.o_s.at[slot], self.c_r.at[q], p.along(first, step, dc=1))

    def finish(self, q):
        slot = lax.rem(q, 2)
        _, owned = self.place_of(q)

        def settle():
            for sem in (self.o_r, self.o_s):
                drain(self.y.at[slot], sem.at[slot])
            drain(self.o.at[slot], self.l_sem.at[slot])

        if owned is None:
            settle()
            return
        on(owned)(settle)

        @on(jnp.logical_not(owned))
        def _():
            drain(self.z.at[slot], self.o_s.at[slot])

        @on(self.lends(q))
        def _():
            drain(self.z.at[slot], self.c_r.at[q])


def kernel(chunks, x_ref, dy_ref, wg, wu, wd, full_gu, full_d, lent, kept, h_ref, spill, dx_ref, out_g, out_u, out_d, *scratch):
    a_v, dy_v, da_v, gu_v, d_v, dgu_v, act_v, kept_v, own, (ss, rs, ld_sem, kept_sem, io_sem, lend_sem), reduces = scratch
    p = Place()
    meet([p.at(dc=1)] + [p.at(dx=side) for side in SIDES] + [p.at(**{axis: step}, dc=dc) for axis in ("dy", "dz") for step in OTHERS for dc in range(2)])
    tokens, d = a_v.shape
    half = tokens // 2
    small = min(BLOCK, half)
    g = Gather(p, chunks, wg, wu, wd, lent, full_gu, full_d, ss, rs)
    parts = [Reduce(p, chunks, kind, own[kind], (out_g, out_u, out_d)[kind], *reduces[kind]) for kind in (2, 0, 1)]
    total = 2 * chunks

    def tiles(start, stop, count, use):
        steps = tokens // small

        @pl.loop(start * steps // count, stop * steps // count)
        def _(i):
            use(rows_at(i * small, small))

    x_copy = pltpu.make_async_copy(x_ref, dy_v, io_sem.at[0])
    x_copy.start()
    g.lend(lend_sem)
    g.x1_wide(0)
    x_copy.wait()

    def first_norm(t):
        a_v[t, :] = normed(dy_v[t, :])
        da_v[t, :] = jnp.zeros((small, d), f32)

    into = (gu_v, d_v)
    tiles(0, 1, 4, first_norm)
    g.settle_lend(lend_sem)
    g.x1_down(0)
    tiles(1, 3, 4, first_norm)
    g.x2(0, WIDE)
    g.x2(0, DOWN)
    g.x1(1)
    tiles(3, 4, 4, first_norm)
    g.yz1(0, WIDE)
    g.yz1(0, DOWN)
    g.x2(1)
    g.x1(2)
    g.yz2(0, WIDE)
    g.yz2(0, DOWN)
    g.yz1(1)
    g.x2(2)
    g.x1(3)
    g.across(0, WIDE)
    g.across(0, DOWN)
    g.yz1(2)
    g.load(0, 0, into, ld_sem, WIDE)
    g.load(0, 0, into, ld_sem, DOWN)
    g.yz2(1)
    g.x2(3)
    g.x1(4)

    def loaded(n, i):
        drain(into[i].at[lax.rem(n, 2)], ld_sem.at[lax.rem(n, 2), i])

    def gather_on(n):
        for i, step in enumerate((g.across, g.yz2, g.yz1, g.x2, g.x1)):
            on(n + i + 1 < total)(functools.partial(step, n + i + 1))

    def forward_part(k, i):
        slot = lax.rem(k, 2)
        t = rows_at(i * half, half)

        @on(k > 0)
        def _():
            drain(kept_v.at[i], kept_sem.at[i])

        kept_v[i] = dot(a_v[t, :], gu_v[slot])
        pltpu.make_async_copy(kept_v.at[i], kept.at[k, t, :], kept_sem.at[i]).start()
        gate, up = kept_v[i, :, :CHUNK], kept_v[i, :, CHUNK:]
        act = (jax.nn.silu(gate) * up).astype(bf16)
        on(i == 0)(lambda: loaded(k, 1))
        da_v[t, :] += dot(act, d_v[slot])

    @pl.loop(0, chunks)
    def _(k):
        on(k > 0)(lambda: gather_on(k))
        loaded(k, 0)

        @pl.loop(0, 2)
        def _(i):
            @on(i == 1)
            def _():
                on(k == 0)(lambda: gather_on(k))
                on(k > 0)(lambda: g.load(k + 1, lax.rem(k + 1, 2), into, ld_sem))

            forward_part(k, i)

        on(k == 0)(lambda: g.load(k + 1, lax.rem(k + 1, 2), into, ld_sem))

    def between(t):
        h = add_up(dy_v[t, :], da_v[t, :].astype(bf16))
        dy_v[t, :] = h
        a_v[t, :] = normed(h)
        da_v[t, :] = jnp.zeros((small, d), f32)
        pltpu.make_async_copy(dy_v.at[t, :], h_ref.at[t, :], io_sem.at[1]).start()

    tiles(0, 1, 1, between)
    drain(dy_v, io_sem.at[1])
    dy_copy = pltpu.make_async_copy(dy_ref, dy_v, io_sem.at[0])
    dy_copy.start()
    for i in range(2):
        drain(kept_v.at[i], kept_sem.at[i])

    def each(step, q):
        for part in parts:
            getattr(part, step)(q)

    def fetch(ref):
        return pltpu.make_async_copy(ref, a_v, io_sem.at[0])

    def keep(t):
        b = lax.rem(t, 2)
        return pltpu.make_async_copy(kept.at[t // 2, rows_at(b * half, half), :], kept_v.at[b], kept_sem.at[b])

    def through_norm(start, stop, then):
        def use(t):
            wide = a_v[t, :].astype(f32)
            scale = scale_of(wide)
            hat = wide * scale
            da = da_v[t, :].astype(bf16).astype(f32)
            back = scale * (da - hat * jnp.mean(da * hat, -1, keepdims=True))
            dy_v[t, :] = add_up(dy_v[t, :], back.astype(bf16))
            da_v[t, :] = jnp.zeros((small, d), f32)
            then(t)

        tiles(start, stop, 2, use)

    def through_gate(t, gate, up, slot):
        dact = dot_nt(dy_v[t, :], d_v[slot]).astype(bf16).astype(f32)
        sig = jax.nn.sigmoid(gate)
        silu = gate * sig
        act_v[t, :] = (silu * up).astype(bf16)
        dgu_v[t, :CHUNK] = (dact * up * (sig * (1 + gate * (1 - sig)))).astype(bf16)
        dgu_v[t, CHUNK:] = (dact * silu).astype(bf16)

    def da_tile(t, slot):
        da_v[t, :] += dot_nt(dgu_v[t, :], gu_v[slot])

    def gate_part(q, slot, i):
        k = lax.rem(q, chunks)

        def layer1(joined):
            t = rows_at(i * half, half)
            if joined:
                da_tile(t, 1 - slot)
            gu = dot(a_v[t, :], gu_v[slot])
            if not joined:
                on(i == 0)(dy_copy.wait)
            through_gate(t, gu[:, :CHUNK], gu[:, CHUNK:], slot)

        def layer0(joined):
            n = (q - chunks) * 2 + i
            keep(n).wait()
            t = rows_at(i * half, half)
            if joined:
                da_tile(t, 1 - slot)
            through_gate(t, kept_v[i, :, :CHUNK], kept_v[i, :, CHUNK:], slot)

            @on(n + 2 < 2 * chunks)
            def _():
                keep(n + 2).start()

        joins = (k > 0) & (q != total - 1)
        for joined in (False, True):
            on((q < chunks) & (joins == joined))(functools.partial(layer1, joined))
            on((q >= chunks) & (q < total) & (joins == joined))(functools.partial(layer0, joined))

    away_copy = pltpu.make_async_copy(dgu_v, spill, io_sem.at[1])

    def back_copy(i):
        t = rows_at(i * half, half)
        return pltpu.make_async_copy(spill.at[t, :], dgu_v.at[t, :], kept_sem.at[i])

    @pl.loop(0, total + 4)
    def _(q):
        slot, side = lax.rem(q, 2), lax.rem(q + chunks, 2)
        busy = q < total
        ahead = chunks + q
        one = (q >= 1) & (q <= total)
        two = (q >= 2) & (q <= total + 1)
        three = (q >= 3) & (q <= total + 2)

        @on(three & (q != total + 1))
        def _():
            each("yz2", q - 3)

        @on(q >= 4)
        def _():
            each("finish", q - 4)

        @pl.loop(0, jnp.where(q == total, 4, jnp.where(q == chunks, 2, 0)))
        def _(i):
            j = lax.rem(i, 2)
            on((q == total) & (i == 1))(lambda: each("x1", q - 1))

            @on(i == 3)
            def _():
                each("yz3", q - 3)
                each("yz1", q - 2)
                each("x2", q - 1)

            on(i >= 2)(back_copy(j).wait)
            da_tile(rows_at(j * half, half), jnp.where(i < 2, 1 - side, side))
            on((q == total) & (i < 2))(back_copy(j).start)

        on(q == total - 1)(away_copy.wait)

        @on(q == chunks)
        def _():
            fetch(h_ref).wait()

            def then(t, sem):
                pltpu.make_async_copy(x_ref.at[t, :], a_v.at[t, :], sem).start()

            for i in range(2):
                through_norm(i, i + 1, functools.partial(then, sem=io_sem.at[i]))

            def again(t):
                a_v[t, :] = normed(a_v[t, :])

            for i in range(2):
                drain(a_v.at[pl.ds(i * half, half), :], io_sem.at[i])
                tiles(i, i + 1, 2, again)

        gather_on(ahead)

        @on(busy)
        def _():
            loaded(ahead, 0)
            loaded(ahead, 1)

        @pl.loop(0, 2)
        def _(i):
            @on((q >= 1) & (q < total) & (i == 1))
            def _():
                each("x1", q - 1)

            gate_part(q, side, i)

        on(q == total - 2)(away_copy.start)

        @on(three & (q != total))
        def _():
            each("yz3", q - 3)

        @on(two & (q != total))
        def _():
            each("yz1", q - 2)

        @on(q + 1 < total)
        def _():
            g.load(ahead + 1, 1 - side, into, ld_sem)

        @on(busy)
        def _():
            own[2][slot] = dot_tn(act_v[...], dy_v[...]).astype(bf16)
            parts[0].pair(q)

        @on(q == total)
        def _():
            fetch(x_ref).wait()
            through_norm(0, 1, lambda t: None)
            each("yz2", q - 2)

        @on(one & (q != total))
        def _():
            each("x2", q - 1)

        @on(busy)
        def _():
            both = dot_tn(a_v[...], dgu_v[...]).astype(bf16)
            own[0][slot] = both[:, :CHUNK]
            own[1][slot] = both[:, CHUNK:]
            for part in parts[1:]:
                part.pair(q)

        @on(q == total)
        def _():
            through_norm(1, 2, lambda t: None)
            pltpu.make_async_copy(dy_v, dx_ref, io_sem.at[0]).start()

        @on(q == chunks - 1)
        def _():
            fetch(h_ref).start()
            keep(0).start()
            keep(1).start()

        @on(q == total - 1)
        def _():
            fetch(x_ref).start()

    pltpu.make_async_copy(dy_v, dx_ref, io_sem.at[0]).wait()


def call(x, dy, wg, wu, wd, chunks):
    tokens, d = x.shape
    layers, rows, _ = wg.shape
    n = layers * chunks
    shapes = [(n, RING, 2, rows, BOTH), (n, RING, 2, HALF, d), (layers, chunks // 2, HALF, d), (chunks, tokens, BOTH), x.shape, (tokens, BOTH), x.shape, wg.shape, wu.shape, wd.shape]
    outs = [jax.ShapeDtypeStruct(shape, f32 if shape == (chunks, tokens, BOTH) else bf16) for shape in shapes]
    scratch = [vmem(tokens, d)] * 2 + [vmem(tokens, d, dtype=f32), vmem(2, d, BOTH), vmem(2, CHUNK, d)]
    scratch += [vmem(tokens, BOTH), vmem(tokens, CHUNK), vmem(2, tokens // 2, BOTH, dtype=f32)]
    scratch += [[vmem(2, d, CHUNK)] * 2 + [vmem(2, CHUNK, d)]]
    scratch += [[dma(5, 2, 2)] * 2 + [dma(2, 2)] + [dma(2)] * 3]
    scratch += [[Reduce.scratch(kind, rows, d, chunks) for kind in range(3)]]
    any_ = pl.BlockSpec(memory_space=pl.ANY)
    ins = (x, dy, wg, wu, wd)
    return pl.pallas_call(
        functools.partial(kernel, chunks),
        in_specs=[any_] * len(ins),
        out_specs=[any_] * len(outs),
        out_shape=outs,
        scratch_shapes=scratch,
        compiler_params=pltpu.CompilerParams(collective_id=0, has_side_effects=True, vmem_limit_bytes=VMEM_LIMIT),
        name="stack",
    )(*ins)


def hand_on_kernel(cuts, *refs):
    count = len(cuts)
    ins, outs, bufs = (refs[i * count : (i + 1) * count] for i in range(3))
    in_sem, out_sem = refs[3 * count :]
    jobs = []
    for src, dst, buf, cut in zip(ins, outs, bufs, cuts):
        size = src.shape[-2] // cut
        wholes = [(l,) for l in range(src.shape[0])] if len(src.shape) > 2 else [()]
        for t in [(*whole, pl.ds(j * size, size)) for whole in wholes for j in range(cut)]:
            i = len(jobs)
            jobs.append((pltpu.make_async_copy(src.at[t], buf.at[t], in_sem.at[i]), pltpu.make_async_copy(buf.at[t], dst.at[t], out_sem.at[i])))
    for come, _ in jobs:
        come.start()
    for come, go in jobs:
        come.wait()
        go.start()
    for _, go in jobs:
        go.wait()


def hand_on(*arrays):
    cuts = [8 if v.ndim == 2 else 3 for v in arrays]
    pieces = sum(cut * (v.shape[0] if v.ndim > 2 else 1) for v, cut in zip(arrays, cuts))
    any_ = pl.BlockSpec(memory_space=pl.ANY)
    return pl.pallas_call(
        functools.partial(hand_on_kernel, cuts),
        in_specs=[any_] * len(arrays),
        out_specs=[any_] * len(arrays),
        out_shape=[jax.ShapeDtypeStruct(v.shape, bf16) for v in arrays],
        scratch_shapes=[vmem(*v.shape) for v in arrays] + [dma(pieces)] * 2,
        name="hand_on",
    )(*arrays)


def solution(mesh):
    def step(x, dy, wg, wu, wd):
        dx, *out = hand_on(*call(x[0], dy[0], wg, wu, wd, wg.shape[2] // CHUNK)[6:])
        return dx[None], *out

    states, cut = P(("rep", "r", "s"), None, None), P(None, "s", None)
    return jax.shard_map(
        step,
        mesh=mesh,
        in_specs=(states, states) + (cut,) * 3,
        out_specs=(states,) + (P("rep", "s", None),) * 3,
        check_vma=False,
    )
```
